32 devices in a mesh: dp: 4 (over y, z), sp: 8 (over x, core).
Axes of the slice: x: 4, y: 2, z: 2, core: 2. Of those that a mesh axis runs over, the one named last changes fastest.
The devices are a block of a 4x4x8 slice.
Arguments:
- x_tok: bfloat16 [32768, 1536], P(('dp', 'sp')), parts along dimension 0
- doc_start: int32 [32768], P(('dp', 'sp')), parts along dimension 0
- w_q: bfloat16 [1536, 24, 64], replicated
- w_k: bfloat16 [1536, 24, 64], replicated
- w_v: bfloat16 [1536, 24, 64], replicated
- w_o: bfloat16 [24, 64, 1536], replicated
- dy_tok: bfloat16 [32768, 1536], P(('dp', 'sp')), parts along dimension 0
Outputs:
- output 1: bfloat16 [32768, 1536], P(('dp', 'sp')), parts along dimension 0
- output 2: bfloat16 [32768, 1536], P(('dp', 'sp')), parts along dimension 0
- output 3: float32 [6144, 24, 64], P('dp'), parts along dimension 0
- output 4: float32 [6144, 24, 64], P('dp'), parts along dimension 0
- output 5: float32 [6144, 24, 64], P('dp'), parts along dimension 0
- output 6: float32 [96, 64, 1536], P('dp'), parts along dimension 0
There are 4 independent parts. The reference program is written for one: setup_inputs(seed, part) draws one part's arguments, and reference() takes and returns one part's arrays. A program takes and returns all parts, laid end to end along the dimension named above; an argument that names none is the same for every part.
All inputs are finite; a program needn't handle non-finite values.
Results may differ from the reference program's by a relative error of at most 0.00188113.
Values are sent between devices in bfloat16 or wider.
A program may use at most 768 MiB of HBM per device.

```python
import math
import jax
import jax.numpy as jnp
from jax import lax

D_MODEL = 1536
HEAD_DIM = 64
TOK_DEV = 1024
SEQ_DEVS = 8

NUM_HEADS = D_MODEL // HEAD_DIM
SEQ_LEN = SEQ_DEVS * TOK_DEV
NUM_BOUNDS = SEQ_DEVS // 2 + 1
SCORE_SCALE = 1.0 / (math.sqrt(HEAD_DIM) * TOK_DEV)


def setup_inputs(seed: int = 0, part: int = 0) -> dict:
    key_list = jax.random.split(jax.random.key(seed), 9)
    k_tok = jax.random.fold_in(key_list[0], part)
    k_tok_mean = jax.random.fold_in(key_list[1], part)
    k_grad = jax.random.fold_in(key_list[2], part)
    k_grad_mean = jax.random.fold_in(key_list[3], part)
    k_doc = jax.random.fold_in(key_list[4], part)
    w_scale = D_MODEL ** -0.5
    x_tok = (jax.random.normal(k_tok, (SEQ_LEN, D_MODEL), jnp.float32)
             + jax.random.normal(k_tok_mean, (1, D_MODEL), jnp.float32)).astype(jnp.bfloat16)
    dy_tok = (jax.random.normal(k_grad, (SEQ_LEN, D_MODEL), jnp.float32)
              + jax.random.normal(k_grad_mean, (1, D_MODEL), jnp.float32)).astype(jnp.bfloat16)
    bound_pos = jax.random.randint(k_doc, (NUM_BOUNDS,), 0, SEQ_LEN)
    doc_start = jnp.zeros((SEQ_LEN,), jnp.int32).at[bound_pos].set(1)
    w_q = (jax.random.normal(key_list[5], (D_MODEL, NUM_HEADS, HEAD_DIM), jnp.float32) * w_scale).astype(jnp.bfloat16)
    w_k = (jax.random.normal(key_list[6], (D_MODEL, NUM_HEADS, HEAD_DIM), jnp.float32) * w_scale).astype(jnp.bfloat16)
    w_v = (jax.random.normal(key_list[7], (D_MODEL, NUM_HEADS, HEAD_DIM), jnp.float32) * w_scale).astype(jnp.bfloat16)
    w_o = (jax.random.normal(key_list[8], (NUM_HEADS, HEAD_DIM, D_MODEL), jnp.float32) * w_scale).astype(jnp.bfloat16)
    return {'x_tok': x_tok, 'doc_start': doc_start, 'w_q': w_q, 'w_k': w_k, 'w_v': w_v, 'w_o': w_o, 'dy_tok': dy_tok}


def block_masks(flag_loc):
    positions = jnp.arange(TOK_DEV)
    seg_ids = jnp.cumsum(flag_loc)
    first_pos = jnp.min(jnp.where(flag_loc > 0, positions, TOK_DEV))
    last_pos = jnp.max(jnp.where(flag_loc > 0, positions, -1))
    head_mask = (positions < first_pos).astype(jnp.float32)
    tail_mask = (positions >= last_pos).astype(jnp.float32)
    same_doc = (seg_ids[:, None] == seg_ids[None, :]) & (positions[None, :] <= positions[:, None])
    doc_gate = (last_pos < 0).astype(jnp.float32)
    return head_mask, tail_mask, same_doc, doc_gate


def reference(x_tok, doc_start, w_q, w_k, w_v, w_o, dy_tok):
    wq_mat = w_q.reshape(D_MODEL, D_MODEL)
    wk_mat = w_k.reshape(D_MODEL, D_MODEL)
    wv_mat = w_v.reshape(D_MODEL, D_MODEL)
    wo_mat = w_o.reshape(D_MODEL, D_MODEL)

    def project(x_loc):
        q_rows = jnp.dot(x_loc, wq_mat, preferred_element_type=jnp.float32).astype(jnp.bfloat16).astype(jnp.float32)
        k_rows = jnp.dot(x_loc, wk_mat, preferred_element_type=jnp.float32).astype(jnp.bfloat16).astype(jnp.float32)
        v_rows = jnp.dot(x_loc, wv_mat, preferred_element_type=jnp.float32).astype(jnp.bfloat16).astype(jnp.float32)
        shape3 = (TOK_DEV, NUM_HEADS, HEAD_DIM)
        return q_rows.reshape(shape3), k_rows.reshape(shape3), v_rows.reshape(shape3)

    def forward_step(fwd_state, step_in):
        x_loc, flag_loc = step_in
        head_mask, tail_mask, same_doc, doc_gate = block_masks(flag_loc)
        q_rows, k_rows, v_rows = project(x_loc)
        scores = jnp.einsum('thk,shk->hts', q_rows, k_rows)
        attn_prob = jnp.where(same_doc[None], scores * SCORE_SCALE, 0.0).astype(jnp.bfloat16).astype(jnp.float32)
        intra_sum = jnp.einsum('hts,shv->thv', attn_prob, v_rows)
        state_low = fwd_state.astype(jnp.bfloat16).astype(jnp.float32)
        inter_sum = jnp.einsum('thk,hkv->thv', q_rows, state_low) * (SCORE_SCALE * head_mask)[:, None, None]
        out_rows = (intra_sum + inter_sum).astype(jnp.bfloat16).reshape(TOK_DEV, D_MODEL)
        y_loc = jnp.dot(out_rows, wo_mat, preferred_element_type=jnp.float32).astype(jnp.bfloat16)
        m_tail = jnp.einsum('shk,shv->hkv', k_rows, v_rows * tail_mask[:, None, None])
        next_state = doc_gate * fwd_state + m_tail
        return next_state, (out_rows, y_loc, fwd_state)

    def backward_step(scan_carry, step_in):
        rev_state, acc_q, acc_k, acc_v, acc_o = scan_carry
        x_loc, flag_loc, dy_loc, out_rows, fwd_state = step_in
        head_mask, tail_mask, same_doc, doc_gate = block_masks(flag_loc)
        q_rows, k_rows, v_rows = project(x_loc)
        scores = jnp.einsum('thk,shk->hts', q_rows, k_rows)
        attn_prob = jnp.where(same_doc[None], scores * SCORE_SCALE, 0.0).astype(jnp.bfloat16).astype(jnp.float32)
        d_out = jnp.dot(dy_loc, wo_mat.T, preferred_element_type=jnp.float32).astype(jnp.bfloat16).astype(jnp.float32)
        d_out = d_out.reshape(TOK_DEV, NUM_HEADS, HEAD_DIM)
        dp_raw = jnp.einsum('thv,shv->hts', d_out, v_rows)
        d_prob = jnp.where(same_doc[None], dp_raw * SCORE_SCALE, 0.0).astype(jnp.bfloat16).astype(jnp.float32)
        state_low = fwd_state.astype(jnp.bfloat16).astype(jnp.float32)
        rev_low = rev_state.astype(jnp.bfloat16).astype(jnp.float32)
        head_col = (SCORE_SCALE * head_mask)[:, None, None]
        tail_col = (SCORE_SCALE * tail_mask)[:, None, None]
        dq_rows = (jnp.einsum('hts,shk->thk', d_prob, k_rows)
                   + jnp.einsum('thv,hkv->thk', d_out, state_low) * head_col).astype(jnp.bfloat16).reshape(TOK_DEV, D_MODEL)
        dk_rows = (jnp.einsum('hts,thk->shk', d_prob, q_rows)
                   + jnp.einsum('shv,hkv->shk', v_rows, rev_low) * tail_col).astype(jnp.bfloat16).reshape(TOK_DEV, D_MODEL)
        dv_rows = (jnp.einsum('hts,thv->shv', attn_prob, d_out)
                   + jnp.einsum('shk,hkv->shv', k_rows, rev_low) * tail_col).astype(jnp.bfloat16).reshape(TOK_DEV, D_MODEL)
        dx_loc = (jnp.dot(dq_rows, wq_mat.T, preferred_element_type=jnp.float32)
                  + jnp.dot(dk_rows, wk_mat.T, preferred_element_type=jnp.float32)
                  + jnp.dot(dv_rows, wv_mat.T, preferred_element_type=jnp.float32)).astype(jnp.bfloat16)
        acc_q = acc_q + jnp.dot(x_loc.T, dq_rows, preferred_element_type=jnp.float32)
        acc_k = acc_k + jnp.dot(x_loc.T, dk_rows, preferred_element_type=jnp.float32)
        acc_v = acc_v + jnp.dot(x_loc.T, dv_rows, preferred_element_type=jnp.float32)
        acc_o = acc_o + jnp.dot(out_rows.T, dy_loc, preferred_element_type=jnp.float32)
        n_head = jnp.einsum('thk,thv->hkv', q_rows, d_out * head_mask[:, None, None])
        next_rev = doc_gate * rev_state + n_head
        return (next_rev, acc_q, acc_k, acc_v, acc_o), dx_loc

    x_blocks = x_tok.reshape(SEQ_DEVS, TOK_DEV, D_MODEL)
    flag_blocks = doc_start.reshape(SEQ_DEVS, TOK_DEV)
    dy_blocks = dy_tok.reshape(SEQ_DEVS, TOK_DEV, D_MODEL)
    zero_state = jnp.zeros((NUM_HEADS, HEAD_DIM, HEAD_DIM), jnp.float32)
    last_state, fwd_outs = lax.scan(forward_step, zero_state, (x_blocks, flag_blocks))
    out_blocks, y_blocks, state_blocks = fwd_outs
    zero_grad = jnp.zeros((D_MODEL, D_MODEL), jnp.float32)
    grad_carry, dx_blocks = lax.scan(backward_step, (zero_state, zero_grad, zero_grad, zero_grad, zero_grad),
                                     (x_blocks, flag_blocks, dy_blocks, out_blocks, state_blocks), reverse=True)
    acc_q = grad_carry[1]
    acc_k = grad_carry[2]
    acc_v = grad_carry[3]
    acc_o = grad_carry[4]
    return (y_blocks.reshape(SEQ_LEN, D_MODEL), dx_blocks.reshape(SEQ_LEN, D_MODEL),
            acc_q.reshape(D_MODEL, NUM_HEADS, HEAD_DIM), acc_k.reshape(D_MODEL, NUM_HEADS, HEAD_DIM),
            acc_v.reshape(D_MODEL, NUM_HEADS, HEAD_DIM), acc_o.reshape(NUM_HEADS, HEAD_DIM, D_MODEL))
```

```python
import functools
import math
import jax
import jax.numpy as jnp
from jax import lax
from jax.experimental import pallas as pl
from jax.experimental.pallas import tpu as pltpu
from jax.sharding import PartitionSpec as P

MESH = pl.DeviceIdType.MESH
BF16 = jnp.bfloat16
F32 = jnp.float32
HEAD = 64
QUAD = 4 * HEAD
BLK = 256
VMEM_CAP = 64 * 1024 * 1024 - 128 * 1024

NN = (((1,), (0,)), ((), ()))
NT = (((1,), (1,)), ((), ()))
TN = (((0,), (0,)), ((), ()))


def mm(lhs, rhs, dims):
    return lax.dot_general(lhs, rhs, dims, preferred_element_type=F32)


def pack_states(full):
    lane = lax.broadcasted_iota(jnp.int32, (HEAD, 2 * HEAD), 1)
    first = jnp.where(lane < HEAD, full[0:HEAD, 0:2 * HEAD], full[HEAD:2 * HEAD, 0:2 * HEAD])
    second = jnp.where(lane < HEAD, full[2 * HEAD:3 * HEAD, 2 * HEAD:], full[3 * HEAD:, 2 * HEAD:])
    return jnp.concatenate([first, second], axis=0)


def spread_states(packed):
    lane = lax.broadcasted_iota(jnp.int32, (HEAD, 2 * HEAD), 1)
    zero = jnp.zeros((HEAD, 2 * HEAD), F32)
    rows = []
    for head in range(4):
        pair = packed[(head // 2) * HEAD:(head // 2 + 1) * HEAD, :]
        own = jnp.where((lane < HEAD) == (head % 2 == 0), pair, 0.0)
        rows.append(jnp.concatenate([own, zero] if head < 2 else [zero, own], axis=1))
    return jnp.concatenate(rows, axis=0)


def proj_kernel(flag_ref, x_ref, dy_ref, wq_ref, wk_ref, wv_ref, wo_ref,
                qt_ref, kt_ref, vt_ref, dot_ref, mt_ref, nt_ref, bound_ref):
    toks = x_ref.shape[0]

    @pl.when(pl.program_id(0) == 0)
    def _():
        lane = lax.broadcasted_iota(jnp.int32, (8, toks), 1)
        flags = jnp.broadcast_to(flag_ref[...], (8, toks))
        last = jnp.where(flags > 0, lane.astype(F32), -1.0)
        step = 1
        while step < toks:
            last = jnp.maximum(last, jnp.where(lane >= step, pltpu.roll(last, step, 1), -1.0))
            step *= 2
        bound_ref[...] = last

    bound = bound_ref[0:1, :]
    last_bound = jnp.max(bound, axis=1, keepdims=True)
    pos = lax.broadcasted_iota(jnp.int32, (1, toks), 1).astype(F32)
    head_row = bound < 0.0
    tail_row = pos >= last_bound
    x_val = x_ref[...]
    q_val = mm(wq_ref[...], x_val, NT).astype(BF16)
    qt_ref[...] = q_val
    k_val = mm(wk_ref[...], x_val, NT).astype(BF16)
    kt_ref[...] = k_val
    v_raw = mm(wv_ref[...], x_val, NT)
    vt_ref[...] = v_raw.astype(BF16)
    mt_ref[...] = pack_states(mm(jnp.where(tail_row, v_raw, 0.0).astype(BF16), k_val, NT))
    d_raw = mm(wo_ref[...], dy_ref[...], NT)
    dot_ref[...] = d_raw.astype(BF16)
    nt_ref[...] = pack_states(mm(jnp.where(head_row, d_raw, 0.0).astype(BF16), q_val, NT))


def project(flags, x_loc, dy_loc, wq, wk, wv, wo):
    toks, width = x_loc.shape
    steps = width // QUAD
    whole = lambda i: (0, 0)
    rows = lambda i: (i, 0)
    act = jax.ShapeDtypeStruct((width, toks), BF16)
    state = jax.ShapeDtypeStruct((width // 2, 2 * HEAD), F32)
    return pl.pallas_call(
        proj_kernel,
        name='project',
        grid=(steps,),
        in_specs=[pl.BlockSpec((1, toks), whole), pl.BlockSpec((toks, width), whole), pl.BlockSpec((toks, width), whole)]
        + [pl.BlockSpec((QUAD, width), rows)] * 4,
        out_specs=[pl.BlockSpec((QUAD, toks), rows)] * 4 + [pl.BlockSpec((QUAD // 2, 2 * HEAD), rows)] * 2
        + [pl.BlockSpec((8, toks), whole)],
        out_shape=[act] * 4 + [state] * 2 + [jax.ShapeDtypeStruct((8, toks), F32)],
        compiler_params=pltpu.CompilerParams(vmem_limit_bytes=VMEM_CAP),
        cost_estimate=pl.CostEstimate(flops=8 * toks * width * width, bytes_accessed=40 * 1024 * 1024, transcendentals=0),
    )(flags.reshape(1, toks), x_loc, dy_loc, wq, wk, wv, wo)


def attn_kernel(devs, scale, qt_ref, kt_ref, vt_ref, dot_ref, mt_ref, nt_ref, bound_ref,
                ot_ref, dvt_ref, dkt_ref, dqt_ref,
                acc_o, acc_q, acc_k, acc_v, s_in, r_in, s_out, r_out, stage, send_sem, recv_sem, out_sem):
    width, toks = qt_ref.shape
    heads = width // HEAD
    nblk = toks // BLK
    me = lax.axis_index('sp')
    barrier = pltpu.get_barrier_semaphore()

    for dev in (lax.rem(me + 1, devs), lax.rem(me + devs - 1, devs)):
        pl.semaphore_signal(barrier, inc=1, device_id={'sp': dev}, device_id_type=MESH)
    pl.semaphore_wait(barrier, 2)

    gate = jnp.where(jnp.max(bound_ref[0:1, :], axis=1, keepdims=True) < 0.0, 1.0, 0.0)
    fwd = pltpu.make_async_remote_copy(src_ref=s_out, dst_ref=s_in, send_sem=send_sem.at[0], recv_sem=recv_sem.at[0],
                                       device_id={'sp': jnp.minimum(me + 1, devs - 1)}, device_id_type=MESH)
    bwd = pltpu.make_async_remote_copy(src_ref=r_out, dst_ref=r_in, send_sem=send_sem.at[1], recv_sem=recv_sem.at[1],
                                       device_id={'sp': jnp.maximum(me - 1, 0)}, device_id_type=MESH)

    @pl.when(me == 0)
    def _():
        s_in[...] = jnp.zeros_like(s_in)
        s_out[...] = mt_ref[...]

    @pl.when(me == devs - 1)
    def _():
        r_in[...] = jnp.zeros_like(r_in)
        r_out[...] = nt_ref[...]

    @pl.when(me == 0)
    def _():
        fwd.start()

    @pl.when(me == devs - 1)
    def _():
        bwd.start()

    s_turn = jnp.maximum((me * heads) // devs - 1, 0)
    r_turn = jnp.maximum(((devs - 1 - me) * heads) // devs - 1, 0)

    def take_fwd():
        fwd.wait_recv()

        @pl.when(me < devs - 1)
        def _():
            s_out[...] = gate * s_in[...] + mt_ref[...]
            fwd.start()

    def take_bwd():
        bwd.wait_recv()

        @pl.when(me > 0)
        def _():
            r_out[...] = gate * r_in[...] + nt_ref[...]
            bwd.start()

    diag = (lax.broadcasted_iota(jnp.int32, (BLK, BLK), 0) <= lax.broadcasted_iota(jnp.int32, (BLK, BLK), 1))
    row_id = lax.broadcasted_iota(jnp.int32, (BLK, BLK), 0).astype(F32)

    def head_step(head, carry):
        base = pl.multiple_of(head * HEAD, HEAD)
        rows = pl.ds(base, HEAD)
        for tb in range(nblk):
            t_cols = pl.ds(tb * BLK, BLK)
            q_val = qt_ref[rows, t_cols]
            d_val = dot_ref[rows, t_cols]
            low = bound_ref[0:1, t_cols]
            o_sum = None
            q_sum = None
            for sb in range(tb + 1):
                s_cols = pl.ds(sb * BLK, BLK)
                k_val = kt_ref[rows, s_cols]
                v_val = vt_ref[rows, s_cols]
                seen = row_id + float(sb * BLK) >= low
                if sb == tb:
                    seen = jnp.logical_and(seen, diag)
                prob = jnp.where(seen, mm(k_val, q_val, TN) * scale, 0.0).astype(BF16)
                d_prob = jnp.where(seen, mm(v_val, d_val, TN) * scale, 0.0).astype(BF16)
                o_part = mm(v_val, prob, NN)
                q_part = mm(k_val, d_prob, NN)
                k_part = mm(q_val, d_prob, NT)
                v_part = mm(d_val, prob, NT)
                o_sum = o_part if o_sum is None else o_sum + o_part
                q_sum = q_part if q_sum is None else q_sum + q_part
                if sb == tb:
                    acc_k[rows, s_cols] = k_part
                    acc_v[rows, s_cols] = v_part
                else:
                    acc_k[rows, s_cols] += k_part
                    acc_v[rows, s_cols] += v_part
            acc_o[rows, t_cols] = o_sum
            acc_q[rows, t_cols] = q_sum
        early = me * 2 < devs

        @pl.when(jnp.logical_and(early, jnp.logical_and(me > 0, head == s_turn)))
        def _():
            take_fwd()

        @pl.when(jnp.logical_and(me < devs - 1, head == r_turn))
        def _():
            take_bwd()

        @pl.when(jnp.logical_and(jnp.logical_not(early), head == s_turn))
        def _():
            take_fwd()
        return carry

    lax.fori_loop(0, heads, head_step, 0)

    @pl.when(me < devs - 1)
    def _():
        fwd.wait_send()

    @pl.when(me > 0)
    def _():
        bwd.wait_send()

    bound = bound_ref[0:1, :]
    last_bound = jnp.max(bound, axis=1, keepdims=True)
    pos = lax.broadcasted_iota(jnp.int32, (1, toks), 1).astype(F32)
    head_row = jnp.where(bound < 0.0, scale, 0.0)
    tail_row = jnp.where(pos >= last_bound, scale, 0.0)
    outs = (ot_ref, dqt_ref, dvt_ref, dkt_ref)

    def out_copy(which, quad, slot):
        return pltpu.make_async_copy(stage.at[slot, which], outs[which].at[pl.ds(quad * QUAD, QUAD)], out_sem.at[slot, which])

    def quad_step(quad, carry):
        slot = lax.rem(quad, 2)

        @pl.when(quad >= 2)
        def _():
            for which in range(4):
                out_copy(which, quad - 2, slot).wait()
        rows = pl.ds(pl.multiple_of(quad * QUAD, QUAD), QUAD)
        packed = pl.ds(pl.multiple_of(quad * (QUAD // 2), QUAD // 2), QUAD // 2)
        s_full = spread_states(s_in[packed, :]).astype(BF16)
        r_full = spread_states(r_in[packed, :]).astype(BF16)
        for tb in range(nblk):
            cols = pl.ds(tb * BLK, BLK)
            h_row = head_row[:, tb * BLK:(tb + 1) * BLK]
            e_row = tail_row[:, tb * BLK:(tb + 1) * BLK]
            stage[slot, 0, :, cols] = (acc_o[rows, cols] + mm(s_full, qt_ref[rows, cols], NN) * h_row).astype(BF16)
            stage[slot, 1, :, cols] = (acc_q[rows, cols] + mm(s_full, dot_ref[rows, cols], TN) * h_row).astype(BF16)
            stage[slot, 2, :, cols] = (acc_v[rows, cols] + mm(r_full, kt_ref[rows, cols], NN) * e_row).astype(BF16)
            stage[slot, 3, :, cols] = (acc_k[rows, cols] + mm(r_full, vt_ref[rows, cols], TN) * e_row).astype(BF16)
        for which in range(4):
            out_copy(which, quad, slot).start()
        return carry

    quads = width // QUAD
    lax.fori_loop(0, quads, quad_step, 0)
    for quad in range(max(quads - 2, 0), quads):
        for which in range(4):
            out_copy(which, quad, quad % 2).wait()


def attend(devs, scale, qt, kt, vt, dot_t, mt, nt, bound):
    width, toks = qt.shape
    act = jax.ShapeDtypeStruct((width, toks), BF16)
    state = pltpu.VMEM(mt.shape, F32)
    return pl.pallas_call(
        functools.partial(attn_kernel, devs, scale),
        name='attend',
        in_specs=[pl.BlockSpec(memory_space=pltpu.VMEM)] * 7,
        out_specs=[pl.BlockSpec(memory_space=pl.ANY)] * 4,
        out_shape=[act] * 4,
        scratch_shapes=[pltpu.VMEM((width, toks), F32)] * 4 + [state] * 4
        + [pltpu.VMEM((2, 4, QUAD, toks), BF16), pltpu.SemaphoreType.DMA((2,)), pltpu.SemaphoreType.DMA((2,)),
           pltpu.SemaphoreType.DMA((2, 4))],
        compiler_params=pltpu.CompilerParams(vmem_limit_bytes=VMEM_CAP, collective_id=0, has_side_effects=True),
        cost_estimate=pl.CostEstimate(flops=12 * toks * toks * width, bytes_accessed=30 * 1024 * 1024, transcendentals=0),
    )(qt, kt, vt, dot_t, mt, nt, bound)


ACC_SLOTS = 8
MSG_SLOTS = 4


def ring_kernel(devs, seg, ot_ref, dvt_ref, dkt_ref, dqt_ref, x_ref, dy_ref, out_ref,
                xy, lhs, part, acc, inbox, xy_sem, lhs_sem, pair_send, pair_recv, rs_send, rs_recv,
                ag_send, ag_recv, fin_sem, peer_send, peer_recv):
    width, toks = ot_ref.shape
    chips = devs // 2
    per = width // seg
    count = 4 * per
    half = seg // 2
    side = seg // 4
    piece = side // chips
    me = lax.axis_index('sp')
    core = lax.rem(me, 2)
    chip = me // 2
    partner = chip * 2 + 1 - core
    targets = (lax.rem(chip + 1, chips) * 2 + core, lax.rem(chip + chips - 1, chips) * 2 + core)

    srcs = (ot_ref, dvt_ref, dkt_ref, dqt_ref)

    def lhs_copy(which, row, slot):
        return pltpu.make_async_copy(srcs[which].at[pl.ds(row, seg)], lhs.at[slot], lhs_sem.at[slot])

    def start_lhs(idx):
        for which in range(4):
            @pl.when(idx // per == which)
            def _():
                lhs_copy(which, pl.multiple_of(lax.rem(idx, per) * seg, seg), lax.rem(idx, 2)).start()

    load_dy = pltpu.make_async_copy(dy_ref, xy.at[0], xy_sem.at[0])
    load_x = pltpu.make_async_copy(x_ref, xy.at[1], xy_sem.at[1])
    load_dy.start()
    load_x.start()
    start_lhs(jnp.int32(0))

    barrier = pltpu.get_barrier_semaphore()
    for dev in (partner,) + targets:
        pl.semaphore_signal(barrier, inc=1, device_id={'sp': dev}, device_id_type=MESH)
    pl.semaphore_wait(barrier, 3)
    load_dy.wait()
    load_x.wait()

    def remote(src, dst, s_sem, r_sem, dev):
        return pltpu.make_async_remote_copy(src_ref=src, dst_ref=dst, send_sem=s_sem, recv_sem=r_sem,
                                            device_id={'sp': dev}, device_id_type=MESH)

    def ring_idx(idx):
        return lax.rem(idx + 4 * chips, chips)

    def pair_copy(idx):
        slot = lax.rem(idx, ACC_SLOTS)
        src = part.at[lax.rem(idx, 2), pl.ds(pl.multiple_of((1 - core) * half, half), half)]
        return remote(src, acc.at[slot], pair_send.at[slot], pair_recv.at[slot], partner)

    def acc_rows(idx, way, chunk):
        return acc.at[lax.rem(idx, ACC_SLOTS), pl.ds(pl.multiple_of(way * side + chunk * piece, piece), piece)]

    def out_rows(idx, owner, way, chunk):
        row = idx * seg + owner * half + way * side + chunk * piece
        return out_ref.at[pl.ds(pl.multiple_of(row, piece), piece)]

    def sent_chunk(way, step):
        return ring_idx(chip - step if way == 0 else chip + step)

    def rs_copy(idx, way, step):
        slot = lax.rem(idx, MSG_SLOTS)
        return remote(acc_rows(idx, way, sent_chunk(way, step)), inbox.at[way, step, slot],
                      rs_send.at[way, step, slot], rs_recv.at[way, step, slot], targets[way])

    def ag_chunk(way, step):
        return ring_idx(chip + 1 - step if way == 0 else chip - 1 + step)

    def ag_copy(idx, way, step):
        slot = lax.rem(idx, MSG_SLOTS)
        rows = out_rows(idx, core, way, ag_chunk(way, step))
        src = acc_rows(idx, way, ag_chunk(way, 0)) if step == 0 else rows
        return remote(src, rows, ag_send.at[way, step, slot], ag_recv.at[way, step, slot], targets[way])

    def fin_copy(idx, way):
        chunk = ag_chunk(way, 0)
        return pltpu.make_async_copy(acc_rows(idx, way, chunk), out_rows(idx, core, way, chunk),
                                     fin_sem.at[way, lax.rem(idx, MSG_SLOTS)])

    def peer_copy(idx, way, step):
        slot = lax.rem(idx, MSG_SLOTS)
        rows = out_rows(idx, core, way, ag_chunk(way, step))
        src = acc_rows(idx, way, ag_chunk(way, 0)) if step == 0 else rows
        return remote(src, rows, peer_send.at[way, step, slot], peer_recv.at[way, step, slot], partner)

    def stage_partial(idx):
        slot = lax.rem(idx, 2)
        lhs_copy(0, 0, slot).wait()

        @pl.when(idx + 1 < count)
        def _():
            start_lhs(idx + 1)
        rhs_id = jnp.minimum(idx // per, 1)
        tile_m = min(256, seg)
        tile_n = 512 if width % 512 == 0 else width

        def tile(step, carry):
            cols = pl.ds(pl.multiple_of(step * tile_n, tile_n), tile_n)
            for row in range(0, seg, tile_m):
                part[slot, row:row + tile_m, cols] = mm(lhs[slot, row:row + tile_m, :], xy[rhs_id, :, cols], NN)
            return carry
        lax.fori_loop(0, width // tile_n, tile, 0)
        pair_copy(idx).start()

    def add_rows(idx, way, step):
        chunk = sent_chunk(way, step)
        rows = pl.ds(pl.multiple_of(way * side + chunk * piece, piece), piece)
        slot = lax.rem(idx, ACC_SLOTS)
        acc[slot, rows, :] = acc[slot, rows, :] + inbox[way, step - 1, lax.rem(idx, MSG_SLOTS)]

    def stage_pair(idx):
        copy = pair_copy(idx)
        copy.wait()
        slot = lax.rem(idx, ACC_SLOTS)

        def add(step, carry):
            rows = pl.ds(pl.multiple_of(step * piece, piece), piece)
            own = pl.ds(pl.multiple_of(core * half + step * piece, piece), piece)
            acc[slot, rows, :] = acc[slot, rows, :] + part[lax.rem(idx, 2), own, :]
            return carry
        lax.fori_loop(0, half // piece, add, 0)
        for way in range(2):
            rs_copy(idx, way, 0).start()

    def stage_reduce(idx, step):
        for way in range(2):
            prev = rs_copy(idx, way, step - 1)
            prev.wait_send()
            prev.wait_recv()
            add_rows(idx, way, step)
            if step < chips - 1:
                rs_copy(idx, way, step).start()
            else:
                ag_copy(idx, way, 0).start()
                peer_copy(idx, way, 0).start()
                fin_copy(idx, way).start()

    def stage_gather(idx, step):
        for way in range(2):
            ag_copy(idx, way, step).wait_send()
            slot = lax.rem(idx, MSG_SLOTS)
            got = out_rows(idx, core, way, ag_chunk(way, step + 1))
            remote(got, got, ag_send.at[way, step, slot], ag_recv.at[way, step, slot], targets[way]).wait_recv()
            if step + 1 < chips - 1:
                ag_copy(idx, way, step + 1).start()
            peer_copy(idx, way, step + 1).start()
            if step == 0:
                fin_copy(idx, way).wait()
            finish_peer(idx, way, step)

    def finish_peer(idx, way, step):
        peer_copy(idx, way, step).wait_send()
        slot = lax.rem(idx, MSG_SLOTS)
        got = out_rows(idx, 1 - core, way, ag_chunk(way, step))
        remote(got, got, peer_send.at[way, step, slot], peer_recv.at[way, step, slot], partner).wait_recv()

    def stage_last(idx):
        for way in range(2):
            finish_peer(idx, way, chips - 1)

    stages = [stage_partial]
    order = [(2 * chips, stage_last)]
    for step in reversed(range(chips - 1)):
        order.append((chips + 1 + step, functools.partial(stage_gather, step=step)))
    for step in reversed(range(1, chips)):
        order.append((1 + step, functools.partial(stage_reduce, step=step)))
    order.append((1, stage_pair))
    order.insert(0, (0, stage_partial))

    def round_step(rnd, carry):
        for delay, stage in order:
            idx = rnd - delay

            @pl.when(jnp.logical_and(idx >= 0, idx < count))
            def _():
                stage(idx)
        return carry

    lax.fori_loop(0, count + 2 * chips, round_step, 0)


def ring_sum(devs, seg, ot, dvt, dkt, dqt, x_loc, dy_loc):
    width, toks = ot.shape
    chips = devs // 2
    piece = seg // 4 // chips
    dma = pltpu.SemaphoreType.DMA
    return pl.pallas_call(
        functools.partial(ring_kernel, devs, seg),
        name='ring_sum',
        in_specs=[pl.BlockSpec(memory_space=pl.ANY)] * 6,
        out_specs=pl.BlockSpec(memory_space=pl.ANY),
        out_shape=jax.ShapeDtypeStruct((4 * width, width), F32),
        scratch_shapes=[
            pltpu.VMEM((2, toks, width), BF16),
            pltpu.VMEM((2, seg, toks), BF16),
            pltpu.VMEM((2, seg, width), F32),
            pltpu.VMEM((ACC_SLOTS, seg // 2, width), F32),
            pltpu.VMEM((2, chips - 1, MSG_SLOTS, piece, width), F32),
            dma((2,)), dma((2,)), dma((ACC_SLOTS,)), dma((ACC_SLOTS,)),
            dma((2, chips - 1, MSG_SLOTS)), dma((2, chips - 1, MSG_SLOTS)),
            dma((2, chips - 1, MSG_SLOTS)), dma((2, chips - 1, MSG_SLOTS)),
            dma((2, MSG_SLOTS)),
            dma((2, chips, MSG_SLOTS)), dma((2, chips, MSG_SLOTS)),
        ],
        compiler_params=pltpu.CompilerParams(vmem_limit_bytes=VMEM_CAP, collective_id=1, has_side_effects=True),
        cost_estimate=pl.CostEstimate(flops=8 * toks * width * width, bytes_accessed=100 * 1024 * 1024, transcendentals=0),
    )(ot, dvt, dkt, dqt, x_loc, dy_loc)


def solution(mesh):
    devs = mesh.shape['sp']

    def device_body(x_loc, flag_loc, w_q, w_k, w_v, w_o, dy_loc):
        toks, width = x_loc.shape
        heads, head_dim = w_q.shape[1], w_q.shape[2]
        scale = 1.0 / (math.sqrt(head_dim) * toks)
        wq, wk, wv = [jnp.transpose(w, (1, 2, 0)).reshape(width, width) for w in (w_q, w_k, w_v)]
        wo = w_o.reshape(width, width)
        qt, kt, vt, dot_t, mt, nt, bound = project(flag_loc, x_loc, dy_loc, wq, wk, wv, wo)
        ot, dvt, dkt, dqt = attend(devs, scale, qt, kt, vt, dot_t, mt, nt, bound)
        y_loc = mm(ot, wo, TN).astype(BF16)
        dx_loc = (mm(dqt, wq, TN) + mm(dkt, wk, TN) + mm(dvt, wv, TN)).astype(BF16)
        seg = width // 3 if width % 3 == 0 else width // 2
        total = ring_sum(devs, seg, ot, dvt, dkt, dqt, x_loc, dy_loc)
        dw_o, dw_v, dw_k, dw_q = [total[i * width:(i + 1) * width].reshape(heads, head_dim, width) for i in range(4)]
        dw_q, dw_k, dw_v = [jnp.transpose(dw, (2, 0, 1)) for dw in (dw_q, dw_k, dw_v)]
        return y_loc, dx_loc, dw_q, dw_k, dw_v, dw_o

    row_spec = P(('dp', 'sp'), None)
    flag_spec = P(('dp', 'sp'))
    w_spec = P(None, None, None)
    dw_spec = P('dp', None, None)
    return jax.shard_map(device_body, mesh=mesh,
                         in_specs=(row_spec, flag_spec, w_spec, w_spec, w_spec, w_spec, row_spec),
                         out_specs=(row_spec, row_spec, dw_spec, dw_spec, dw_spec, dw_spec),
                         check_vma=False)
```

```python
import functools
import math
import jax
import jax.numpy as jnp
from jax import lax
from jax.experimental import pallas as pl
from jax.experimental.pallas import tpu as pltpu
from jax.sharding import PartitionSpec as P

MESH = pl.DeviceIdType.MESH
BF16 = jnp.bfloat16
F32 = jnp.float32
HEAD = 64
QUAD = 4 * HEAD
BLK = 256
VMEM_CAP = 64 * 1024 * 1024 - 128 * 1024
ACC_SLOTS = 8
MSG_SLOTS = 4

NN = (((1,), (0,)), ((), ()))
NT = (((1,), (1,)), ((), ()))
TN = (((0,), (0,)), ((), ()))


def mm(lhs, rhs, dims):
    return lax.dot_general(lhs, rhs, dims, preferred_element_type=F32)


def pack_states(full):
    lane = lax.broadcasted_iota(jnp.int32, (HEAD, 2 * HEAD), 1)
    first = jnp.where(lane < HEAD, full[0:HEAD, 0:2 * HEAD], full[HEAD:2 * HEAD, 0:2 * HEAD])
    second = jnp.where(lane < HEAD, full[2 * HEAD:3 * HEAD, 2 * HEAD:], full[3 * HEAD:, 2 * HEAD:])
    return jnp.concatenate([first, second], axis=0)


def spread_states(packed):
    lane = lax.broadcasted_iota(jnp.int32, (HEAD, 2 * HEAD), 1)
    zero = jnp.zeros((HEAD, 2 * HEAD), F32)
    rows = []
    for head in range(4):
        pair = packed[(head // 2) * HEAD:(head // 2 + 1) * HEAD, :]
        own = jnp.where((lane < HEAD) == (head % 2 == 0), pair, 0.0)
        rows.append(jnp.concatenate([own, zero] if head < 2 else [zero, own], axis=1))
    return jnp.concatenate(rows, axis=0)


def fused_kernel(devs, scale, flag_ref, x_ref, dy_ref, wq_ref, wk_ref, wv_ref, wo_ref,
                 out_ref, ot_ref, dqt_ref, dvt_ref, dkt_ref,
                 xy, wbuf, qt, kt, vt, dt, mt, nt, s_in, r_in, s_out, r_out, bound_ref, raw, lhs, part, acc, inbox,
                 xy_sem, w_sem, act_sem, chain_send, chain_recv, pair_send, pair_recv, rs_send, rs_recv,
                 ag_send, ag_recv, fin_sem, peer_send, peer_recv):
    width, toks = qt.shape
    nquad = width // QUAD
    nblk = toks // BLK
    seg = QUAD
    count = 4 * nquad
    chips = devs // 2
    half = seg // 2
    side = seg // 4
    piece = side // chips
    me = lax.axis_index('sp')
    core = lax.rem(me, 2)
    chip = me // 2
    partner = chip * 2 + 1 - core
    targets = (lax.rem(chip + 1, chips) * 2 + core, lax.rem(chip + chips - 1, chips) * 2 + core)
    up = lax.rem(me + 1, devs)
    down = lax.rem(me + devs - 1, devs)

    load_x = pltpu.make_async_copy(x_ref, xy.at[1], xy_sem.at[1])
    load_dy = pltpu.make_async_copy(dy_ref, xy.at[0], xy_sem.at[0])
    load_x.start()

    def w_copies(tick, kv):
        slot = lax.rem(tick, 2)
        rows = pl.ds(pl.multiple_of(lax.rem(tick, nquad) * QUAD, QUAD), QUAD)
        pair = (wk_ref, wv_ref) if kv else (wq_ref, wo_ref)
        return [pltpu.make_async_copy(ref.at[rows], wbuf.at[slot, i], w_sem.at[slot, i]) for i, ref in enumerate(pair)]

    def start_w(tick):
        @pl.when(tick < nquad)
        def _():
            for copy in w_copies(tick, True):
                copy.start()

        @pl.when(jnp.logical_and(tick >= nquad, tick < 2 * nquad))
        def _():
            for copy in w_copies(tick, False):
                copy.start()

    start_w(jnp.int32(0))
    load_dy.start()

    barrier = pltpu.get_barrier_semaphore()
    for dev in (up, down, partner) + targets:
        pl.semaphore_signal(barrier, inc=1, device_id={'sp': dev}, device_id_type=MESH)

    lane = lax.broadcasted_iota(jnp.int32, (8, toks), 1)
    last = jnp.where(jnp.broadcast_to(flag_ref[...], (8, toks)) > 0, lane.astype(F32), -1.0)
    step = 1
    while step < toks:
        last = jnp.maximum(last, jnp.where(lane >= step, pltpu.roll(last, step, 1), -1.0))
        step *= 2
    bound_ref[...] = last
    bound = bound_ref[0:1, :]
    last_bound = jnp.max(bound, axis=1, keepdims=True)
    pos = lax.broadcasted_iota(jnp.int32, (1, toks), 1).astype(F32)
    gate = jnp.where(last_bound < 0.0, 1.0, 0.0)
    diag = (lax.broadcasted_iota(jnp.int32, (BLK, BLK), 0) <= lax.broadcasted_iota(jnp.int32, (BLK, BLK), 1))
    row_id = lax.broadcasted_iota(jnp.int32, (BLK, BLK), 0).astype(F32)

    pl.semaphore_wait(barrier, 5)
    load_x.wait()

    def quad_rows(quad):
        return pl.ds(pl.multiple_of(quad * QUAD, QUAD), QUAD)

    def pack_rows(quad):
        return pl.ds(pl.multiple_of(quad * (QUAD // 2), QUAD // 2), QUAD // 2)

    def project_kv(tick):
        slot = lax.rem(tick, 2)
        for copy in w_copies(tick, True):
            copy.wait()
        start_w(tick + 1)
        x_val = xy[1]
        k_val = mm(wbuf[slot, 0], x_val, NT).astype(BF16)
        kt[quad_rows(tick), :] = k_val
        v_raw = mm(wbuf[slot, 1], x_val, NT)
        vt[quad_rows(tick), :] = v_raw.astype(BF16)
        tail = pos >= last_bound
        mt[pack_rows(tick), :] = pack_states(mm(jnp.where(tail, v_raw, 0.0).astype(BF16), k_val, NT))

    def project_qd(tick):
        slot = lax.rem(tick, 2)
        quad = tick - nquad
        for copy in w_copies(tick, False):
            copy.wait()
        start_w(tick + 1)

        @pl.when(quad == 0)
        def _():
            load_dy.wait()
        q_val = mm(wbuf[slot, 0], xy[1], NT).astype(BF16)
        qt[quad_rows(quad), :] = q_val
        d_raw = mm(wbuf[slot, 1], xy[0], NT)
        dt[quad_rows(quad), :] = d_raw.astype(BF16)
        nt[pack_rows(quad), :] = pack_states(mm(jnp.where(bound < 0.0, d_raw, 0.0).astype(BF16), q_val, NT))

    def chain_copy(way, quad):
        rows = pack_rows(quad)
        src, dst, dev = ((s_out, s_in, up), (r_out, r_in, down))[way]
        return pltpu.make_async_remote_copy(src_ref=src.at[rows], dst_ref=dst.at[rows], send_sem=chain_send.at[way, quad],
                                            recv_sem=chain_recv.at[way, quad], device_id={'sp': dev}, device_id_type=MESH)

    def chain_step(way, quad, first, final):
        rows = pack_rows(quad)
        own, got, nxt = ((mt, s_in, s_out), (nt, r_in, r_out))[way]

        @pl.when(first)
        def _():
            got[rows, :] = jnp.zeros((QUAD // 2, 2 * HEAD), F32)

        @pl.when(jnp.logical_not(first))
        def _():
            chain_copy(way, quad).wait_recv()

        @pl.when(jnp.logical_not(final))
        def _():
            nxt[rows, :] = gate * got[rows, :] + own[rows, :]
            chain_copy(way, quad).start()

    def remote(src, dst, s_sem, r_sem, dev):
        return pltpu.make_async_remote_copy(src_ref=src, dst_ref=dst, send_sem=s_sem, recv_sem=r_sem,
                                            device_id={'sp': dev}, device_id_type=MESH)

    def ring_idx(idx):
        return lax.rem(idx + 4 * chips, chips)

    def pair_copy(idx):
        slot = lax.rem(idx, ACC_SLOTS)
        src = part.at[lax.rem(idx, 2), pl.ds(pl.multiple_of((1 - core) * half, half), half)]
        return remote(src, acc.at[slot], pair_send.at[slot], pair_recv.at[slot], partner)

    def acc_rows(idx, way, chunk):
        return acc.at[lax.rem(idx, ACC_SLOTS), pl.ds(pl.multiple_of(way * side + chunk * piece, piece), piece)]

    def out_rows(idx, owner, way, chunk):
        row = idx * seg + owner * half + way * side + chunk * piece
        return out_ref.at[pl.ds(pl.multiple_of(row, piece), piece)]

    def sent_chunk(way, step):
        return ring_idx(chip - step if way == 0 else chip + step)

    def rs_copy(idx, way, step):
        slot = lax.rem(idx, MSG_SLOTS)
        return remote(acc_rows(idx, way, sent_chunk(way, step)), inbox.at[way, step, slot],
                      rs_send.at[way, step, slot], rs_recv.at[way, step, slot], targets[way])

    def ag_chunk(way, step):
        return ring_idx(chip + 1 - step if way == 0 else chip - 1 + step)

    def ag_copy(idx, way, step):
        slot = lax.rem(idx, MSG_SLOTS)
        rows = out_rows(idx, core, way, ag_chunk(way, step))
        src = acc_rows(idx, way, ag_chunk(way, 0)) if step == 0 else rows
        return remote(src, rows, ag_send.at[way, step, slot], ag_recv.at[way, step, slot], targets[way])

    def fin_copy(idx, way):
        chunk = ag_chunk(way, 0)
        return pltpu.make_async_copy(acc_rows(idx, way, chunk), out_rows(idx, core, way, chunk),
                                     fin_sem.at[way, lax.rem(idx, MSG_SLOTS)])

    def peer_copy(idx, way, step):
        slot = lax.rem(idx, MSG_SLOTS)
        rows = out_rows(idx, core, way, ag_chunk(way, step))
        src = acc_rows(idx, way, ag_chunk(way, 0)) if step == 0 else rows
        return remote(src, rows, peer_send.at[way, step, slot], peer_recv.at[way, step, slot], partner)


    acts = (ot_ref, dqt_ref, dvt_ref, dkt_ref)

    def act_copy(idx, kind):
        slot = lax.rem(idx, 2)
        return pltpu.make_async_copy(lhs.at[slot], acts[kind].at[quad_rows(lax.rem(idx, nquad))], act_sem.at[slot])

    def unit(idx, kind):
        quad = lax.rem(idx, nquad)
        slot = lax.rem(idx, 2)
        by_query = kind < 2
        left, right = (kt, qt) if kind % 2 == 0 else (vt, dt)
        value = (vt, kt, dt, qt)[kind]

        def head_step(head, carry):
            rows = pl.ds(pl.multiple_of(quad * QUAD + head * HEAD, HEAD), HEAD)
            for ob in range(nblk):
                total = None
                for ib in (range(ob + 1) if by_query else range(ob, nblk)):
                    tb, sb = (ob, ib) if by_query else (ib, ob)
                    t_cols, s_cols = pl.ds(tb * BLK, BLK), pl.ds(sb * BLK, BLK)
                    seen = row_id + float(sb * BLK) >= bound_ref[0:1, t_cols]
                    if sb == tb:
                        seen = jnp.logical_and(seen, diag)
                    prob = jnp.where(seen, mm(left[rows, s_cols], right[rows, t_cols], TN) * scale, 0.0).astype(BF16)
                    if by_query:
                        part_sum = mm(value[rows, s_cols], prob, NN)
                    else:
                        part_sum = mm(value[rows, t_cols], prob, NT)
                    total = part_sum if total is None else total + part_sum
                raw[pl.ds(pl.multiple_of(head * HEAD, HEAD), HEAD), ob * BLK:(ob + 1) * BLK] = total
            return carry

        lax.fori_loop(0, QUAD // HEAD, head_step, 0)
        state = s_in if by_query else r_in
        full = spread_states(state[pack_rows(quad), :]).astype(BF16)
        other = (qt, dt, kt, vt)[kind]
        dims = NN if kind % 2 == 0 else TN
        weight = jnp.where(bound < 0.0, scale, 0.0) if by_query else jnp.where(pos >= last_bound, scale, 0.0)
        for tb in range(nblk):
            cols = pl.ds(tb * BLK, BLK)
            extra = mm(full, other[quad_rows(quad), cols], dims) * weight[:, tb * BLK:(tb + 1) * BLK]
            lhs[slot, :, cols] = (raw[:, cols] + extra).astype(BF16)
        act_copy(idx, kind).start()

    def stage_partial(idx):
        slot = lax.rem(idx, 2)

        @pl.when(idx >= 2)
        def _():
            act_copy(idx, 0).wait()
        for kind in range(4):
            @pl.when(idx // nquad == kind)
            def _():
                unit(idx, kind)
        rhs_id = jnp.minimum(idx // nquad, 1)
        tile_n = 512 if width % 512 == 0 else width

        def tile(step, carry):
            cols = pl.ds(pl.multiple_of(step * tile_n, tile_n), tile_n)
            part[slot, :, cols] = mm(lhs[slot], xy[rhs_id, :, cols], NN)
            return carry
        lax.fori_loop(0, width // tile_n, tile, 0)
        pair_copy(idx).start()

    def add_rows(idx, way, step):
        chunk = sent_chunk(way, step)
        rows = pl.ds(pl.multiple_of(way * side + chunk * piece, piece), piece)
        slot = lax.rem(idx, ACC_SLOTS)
        acc[slot, rows, :] = acc[slot, rows, :] + inbox[way, step - 1, lax.rem(idx, MSG_SLOTS)]

    def stage_pair(idx):
        copy = pair_copy(idx)
        copy.wait()
        slot = lax.rem(idx, ACC_SLOTS)

        def add(step, carry):
            rows = pl.ds(pl.multiple_of(step * piece, piece), piece)
            own = pl.ds(pl.multiple_of(core * half + step * piece, piece), piece)
            acc[slot, rows, :] = acc[slot, rows, :] + part[lax.rem(idx, 2), own, :]
            return carry
        lax.fori_loop(0, half // piece, add, 0)
        for way in range(2):
            rs_copy(idx, way, 0).start()

    def stage_reduce(idx, step):
        for way in range(2):
            prev = rs_copy(idx, way, step - 1)
            prev.wait_send()
            prev.wait_recv()
            add_rows(idx, way, step)
            if step < chips - 1:
                rs_copy(idx, way, step).start()
            else:
                ag_copy(idx, way, 0).start()
                peer_copy(idx, way, 0).start()
                fin_copy(idx, way).start()

    def stage_gather(idx, step):
        for way in range(2):
            ag_copy(idx, way, step).wait_send()
            slot = lax.rem(idx, MSG_SLOTS)
            got = out_rows(idx, core, way, ag_chunk(way, step + 1))
            remote(got, got, ag_send.at[way, step, slot], ag_recv.at[way, step, slot], targets[way]).wait_recv()
            if step + 1 < chips - 1:
                ag_copy(idx, way, step + 1).start()
            peer_copy(idx, way, step + 1).start()
            if step == 0:
                fin_copy(idx, way).wait()
            finish_peer(idx, way, step)

    def finish_peer(idx, way, step):
        peer_copy(idx, way, step).wait_send()
        slot = lax.rem(idx, MSG_SLOTS)
        got = out_rows(idx, 1 - core, way, ag_chunk(way, step))
        remote(got, got, peer_send.at[way, step, slot], peer_recv.at[way, step, slot], partner).wait_recv()

    def stage_last(idx):
        for way in range(2):
            finish_peer(idx, way, chips - 1)

    order = [(2 * chips, stage_last)]
    for step in reversed(range(chips - 1)):
        order.append((chips + 1 + step, functools.partial(stage_gather, step=step)))
    for step in reversed(range(1, chips)):
        order.append((1 + step, functools.partial(stage_reduce, step=step)))
    order.append((1, stage_pair))
    order.append((0, stage_partial))
    lead = max(devs - 1, nquad)

    def tick_step(tick, carry):
        @pl.when(tick < nquad)
        def _():
            project_kv(tick)

        @pl.when(jnp.logical_and(tick >= nquad, tick < 2 * nquad))
        def _():
            project_qd(tick)
        s_quad = tick - me
        r_quad = tick - nquad - (devs - 1 - me)

        @pl.when(jnp.logical_and(s_quad >= 0, s_quad < nquad))
        def _():
            chain_step(0, s_quad, me == 0, me == devs - 1)

        @pl.when(jnp.logical_and(r_quad >= 0, r_quad < nquad))
        def _():
            chain_step(1, r_quad, me == devs - 1, me == 0)
        for delay, stage in order:
            idx = tick - lead - delay

            @pl.when(jnp.logical_and(idx >= 0, idx < count))
            def _():
                stage(idx)
        return carry

    lax.fori_loop(0, lead + count + 2 * chips, tick_step, 0)
    for idx in range(count - 2, count):
        act_copy(jnp.int32(idx), 3).wait()

    def chain_end(quad, carry):
        @pl.when(me < devs - 1)
        def _():
            chain_copy(0, quad).wait_send()

        @pl.when(me > 0)
        def _():
            chain_copy(1, quad).wait_send()
        return carry
    lax.fori_loop(0, nquad, chain_end, 0)


def fused(devs, scale, flags, x_loc, dy_loc, wq, wk, wv, wo):
    toks, width = x_loc.shape
    chips = devs // 2
    nquad = width // QUAD
    piece = QUAD // 4 // chips
    dma = pltpu.SemaphoreType.DMA
    act = jax.ShapeDtypeStruct((width, toks), BF16)
    state = pltpu.VMEM((width // 2, 2 * HEAD), F32)
    ring = (2, chips - 1, MSG_SLOTS)
    return pl.pallas_call(
        functools.partial(fused_kernel, devs, scale),
        name='fused',
        in_specs=[pl.BlockSpec(memory_space=pltpu.VMEM)] + [pl.BlockSpec(memory_space=pl.ANY)] * 6,
        out_specs=[pl.BlockSpec(memory_space=pl.ANY)] * 5,
        out_shape=[jax.ShapeDtypeStruct((4 * width, width), F32)] + [act] * 4,
        scratch_shapes=[
            pltpu.VMEM((2, toks, width), BF16),
            pltpu.VMEM((2, 2, QUAD, width), BF16),
            *[pltpu.VMEM((width, toks), BF16)] * 4,
            *[state] * 6,
            pltpu.VMEM((8, toks), F32),
            pltpu.VMEM((QUAD, toks), F32),
            pltpu.VMEM((2, QUAD, toks), BF16),
            pltpu.VMEM((2, QUAD, width), F32),
            pltpu.VMEM((ACC_SLOTS, QUAD // 2, width), F32),
            pltpu.VMEM((2, chips - 1, MSG_SLOTS, piece, width), F32),
            dma((2,)), dma((2, 2)), dma((2,)), dma((2, nquad)), dma((2, nquad)), dma((ACC_SLOTS,)), dma((ACC_SLOTS,)),
            dma(ring), dma(ring), dma(ring), dma(ring), dma((2, MSG_SLOTS)),
            dma((2, chips, MSG_SLOTS)), dma((2, chips, MSG_SLOTS)),
        ],
        compiler_params=pltpu.CompilerParams(vmem_limit_bytes=VMEM_CAP, collective_id=0, has_side_effects=True),
        cost_estimate=pl.CostEstimate(flops=24 * toks * width * width, bytes_accessed=150 * 1024 * 1024, transcendentals=0),
    )(flags.reshape(1, toks), x_loc, dy_loc, wq, wk, wv, wo)


def solution(mesh):
    devs = mesh.shape['sp']

    def device_body(x_loc, flag_loc, w_q, w_k, w_v, w_o, dy_loc):
        toks, width = x_loc.shape
        heads, head_dim = w_q.shape[1], w_q.shape[2]
        scale = 1.0 / (math.sqrt(head_dim) * toks)
        wq, wk, wv = [jnp.transpose(w, (1, 2, 0)).reshape(width, width) for w in (w_q, w_k, w_v)]
        wo = w_o.reshape(width, width)
        total, ot, dqt, dvt, dkt = fused(devs, scale, flag_loc, x_loc, dy_loc, wq, wk, wv, wo)
        y_loc = mm(ot, wo, TN).astype(BF16)
        dx_loc = (mm(dqt, wq, TN) + mm(dkt, wk, TN) + mm(dvt, wv, TN)).astype(BF16)
        dw_o, dw_q, dw_v, dw_k = [total[i * width:(i + 1) * width].reshape(heads, head_dim, width) for i in range(4)]
        dw_q, dw_k, dw_v = [jnp.transpose(dw, (2, 0, 1)) for dw in (dw_q, dw_k, dw_v)]
        return y_loc, dx_loc, dw_q, dw_k, dw_v, dw_o

    row_spec = P(('dp', 'sp'), None)
    flag_spec = P(('dp', 'sp'))
    w_spec = P(None, None, None)
    dw_spec = P('dp', None, None)
    return jax.shard_map(device_body, mesh=mesh,
                         in_specs=(row_spec, flag_spec, w_spec, w_spec, w_spec, w_spec, row_spec),
                         out_specs=(row_spec, row_spec, dw_spec, dw_spec, dw_spec, dw_spec),
                         check_vma=False)
```

```python
import functools
import math
import jax
import jax.numpy as jnp
from jax import lax
from jax.experimental import pallas as pl
from jax.experimental.pallas import tpu as pltpu
from jax.sharding import PartitionSpec as P

MESH = pl.DeviceIdType.MESH
BF16 = jnp.bfloat16
F32 = jnp.float32
HEAD = 64
QUAD = 4 * HEAD
BLK = 256
VMEM_CAP = 64 * 1024 * 1024 - 128 * 1024
ACC_SLOTS = 8
MSG_SLOTS = 4

NN = (((1,), (0,)), ((), ()))
NT = (((1,), (1,)), ((), ()))
TN = (((0,), (0,)), ((), ()))


def mm(lhs, rhs, dims):
    return lax.dot_general(lhs, rhs, dims, preferred_element_type=F32)


def pack_states(full):
    lane = lax.broadcasted_iota(jnp.int32, (HEAD, 2 * HEAD), 1)
    first = jnp.where(lane < HEAD, full[0:HEAD, 0:2 * HEAD], full[HEAD:2 * HEAD, 0:2 * HEAD])
    second = jnp.where(lane < HEAD, full[2 * HEAD:3 * HEAD, 2 * HEAD:], full[3 * HEAD:, 2 * HEAD:])
    return jnp.concatenate([first, second], axis=0)


def spread_states(packed):
    lane = lax.broadcasted_iota(jnp.int32, (HEAD, 2 * HEAD), 1)
    zero = jnp.zeros((HEAD, 2 * HEAD), F32)
    rows = []
    for head in range(4):
        pair = packed[(head // 2) * HEAD:(head // 2 + 1) * HEAD, :]
        own = jnp.where((lane < HEAD) == (head % 2 == 0), pair, 0.0)
        rows.append(jnp.concatenate([own, zero] if head < 2 else [zero, own], axis=1))
    return jnp.concatenate(rows, axis=0)


def fused_kernel(devs, scale, flag_ref, x_ref, dy_ref, wq_ref, wk_ref, wv_ref, wo_ref,
                 out_ref, y_ref, dx_ref,
                 xy, wbuf, qt, kt, vt, dt, mt, nt, s_in, r_in, s_out, r_out, bound_ref, raw, lhs, ot, part, acc, inbox, y_acc, dx_acc, row_out,
                 xy_sem, w_sem, row_sem, chain_send, chain_recv, pair_send, pair_recv, rs_send, rs_recv,
                 ag_send, ag_recv, fin_sem, peer_send, peer_recv):
    width, toks = qt.shape
    nquad = width // QUAD
    nblk = toks // BLK
    seg = QUAD
    count = 4 * nquad
    chips = devs // 2
    half = seg // 2
    side = seg // 4
    piece = side // chips
    me = lax.axis_index('sp')
    core = lax.rem(me, 2)
    chip = me // 2
    partner = chip * 2 + 1 - core
    targets = (lax.rem(chip + 1, chips) * 2 + core, lax.rem(chip + chips - 1, chips) * 2 + core)
    up = lax.rem(me + 1, devs)
    down = lax.rem(me + devs - 1, devs)

    load_x = pltpu.make_async_copy(x_ref, xy.at[1], xy_sem.at[1])
    load_dy = pltpu.make_async_copy(dy_ref, xy.at[0], xy_sem.at[0])
    load_x.start()

    def w_copies(tick, kv):
        slot = lax.rem(tick, 2)
        rows = pl.ds(pl.multiple_of(lax.rem(tick, nquad) * QUAD, QUAD), QUAD)
        pair = (wk_ref, wv_ref) if kv else (wq_ref, wo_ref)
        return [pltpu.make_async_copy(ref.at[rows], wbuf.at[slot, i], w_sem.at[slot, i]) for i, ref in enumerate(pair)]

    def start_w(tick):
        @pl.when(tick < nquad)
        def _():
            for copy in w_copies(tick, True):
                copy.start()

        @pl.when(jnp.logical_and(tick >= nquad, tick < 2 * nquad))
        def _():
            for copy in w_copies(tick, False):
                copy.start()

    start_w(jnp.int32(0))
    load_dy.start()

    barrier = pltpu.get_barrier_semaphore()
    for dev in (up, down, partner) + targets:
        pl.semaphore_signal(barrier, inc=1, device_id={'sp': dev}, device_id_type=MESH)

    lane = lax.broadcasted_iota(jnp.int32, (8, toks), 1)
    last = jnp.where(jnp.broadcast_to(flag_ref[...], (8, toks)) > 0, lane.astype(F32), -1.0)
    step = 1
    while step < toks:
        last = jnp.maximum(last, jnp.where(lane >= step, pltpu.roll(last, step, 1), -1.0))
        step *= 2
    bound_ref[...] = last
    bound = bound_ref[0:1, :]
    last_bound = jnp.max(bound, axis=1, keepdims=True)
    pos = lax.broadcasted_iota(jnp.int32, (1, toks), 1).astype(F32)
    gate = jnp.where(last_bound < 0.0, 1.0, 0.0)
    diag = (lax.broadcasted_iota(jnp.int32, (BLK, BLK), 0) <= lax.broadcasted_iota(jnp.int32, (BLK, BLK), 1))
    row_id = lax.broadcasted_iota(jnp.int32, (BLK, BLK), 0).astype(F32)

    pl.semaphore_wait(barrier, 5)
    load_x.wait()

    def quad_rows(quad):
        return pl.ds(pl.multiple_of(quad * QUAD, QUAD), QUAD)

    def pack_rows(quad):
        return pl.ds(pl.multiple_of(quad * (QUAD // 2), QUAD // 2), QUAD // 2)

    def project_kv(tick):
        slot = lax.rem(tick, 2)
        for copy in w_copies(tick, True):
            copy.wait()
        start_w(tick + 1)
        x_val = xy[1]
        k_val = mm(wbuf[slot, 0], x_val, NT).astype(BF16)
        kt[quad_rows(tick), :] = k_val
        v_raw = mm(wbuf[slot, 1], x_val, NT)
        vt[quad_rows(tick), :] = v_raw.astype(BF16)
        tail = pos >= last_bound
        mt[pack_rows(tick), :] = pack_states(mm(jnp.where(tail, v_raw, 0.0).astype(BF16), k_val, NT))

    def project_qd(tick):
        slot = lax.rem(tick, 2)
        quad = tick - nquad
        for copy in w_copies(tick, False):
            copy.wait()
        start_w(tick + 1)

        @pl.when(quad == 0)
        def _():
            load_dy.wait()
        q_val = mm(wbuf[slot, 0], xy[1], NT).astype(BF16)
        qt[quad_rows(quad), :] = q_val
        d_raw = mm(wbuf[slot, 1], xy[0], NT)
        dt[quad_rows(quad), :] = d_raw.astype(BF16)
        nt[pack_rows(quad), :] = pack_states(mm(jnp.where(bound < 0.0, d_raw, 0.0).astype(BF16), q_val, NT))

    def chain_copy(way, quad):
        rows = pack_rows(quad)
        src, dst, dev = ((s_out, s_in, up), (r_out, r_in, down))[way]
        return pltpu.make_async_remote_copy(src_ref=src.at[rows], dst_ref=dst.at[rows], send_sem=chain_send.at[way, quad],
                                            recv_sem=chain_recv.at[way, quad], device_id={'sp': dev}, device_id_type=MESH)

    def chain_step(way, quad, first, final):
        rows = pack_rows(quad)
        own, got, nxt = ((mt, s_in, s_out), (nt, r_in, r_out))[way]

        @pl.when(first)
        def _():
            got[rows, :] = jnp.zeros((QUAD // 2, 2 * HEAD), F32)

        @pl.when(jnp.logical_not(first))
        def _():
            chain_copy(way, quad).wait_recv()

        @pl.when(jnp.logical_not(final))
        def _():
            nxt[rows, :] = gate * got[rows, :] + own[rows, :]
            chain_copy(way, quad).start()

    def remote(src, dst, s_sem, r_sem, dev):
        return pltpu.make_async_remote_copy(src_ref=src, dst_ref=dst, send_sem=s_sem, recv_sem=r_sem,
                                            device_id={'sp': dev}, device_id_type=MESH)

    def ring_idx(idx):
        return lax.rem(idx + 4 * chips, chips)

    def pair_copy(idx):
        slot = lax.rem(idx, ACC_SLOTS)
        src = part.at[lax.rem(idx, 2), pl.ds(pl.multiple_of((1 - core) * half, half), half)]
        return remote(src, acc.at[slot], pair_send.at[slot], pair_recv.at[slot], partner)

    def acc_rows(idx, way, chunk):
        return acc.at[lax.rem(idx, ACC_SLOTS), pl.ds(pl.multiple_of(way * side + chunk * piece, piece), piece)]

    def out_rows(idx, owner, way, chunk):
        row = idx * seg + owner * half + way * side + chunk * piece
        return out_ref.at[pl.ds(pl.multiple_of(row, piece), piece)]

    def sent_chunk(way, step):
        return ring_idx(chip - step if way == 0 else chip + step)

    def rs_copy(idx, way, step):
        slot = lax.rem(idx, MSG_SLOTS)
        return remote(acc_rows(idx, way, sent_chunk(way, step)), inbox.at[way, step, slot],
                      rs_send.at[way, step, slot], rs_recv.at[way, step, slot], targets[way])

    def ag_chunk(way, step):
        return ring_idx(chip + 1 - step if way == 0 else chip - 1 + step)

    def ag_copy(idx, way, step):
        slot = lax.rem(idx, MSG_SLOTS)
        rows = out_rows(idx, core, way, ag_chunk(way, step))
        src = acc_rows(idx, way, ag_chunk(way, 0)) if step == 0 else rows
        return remote(src, rows, ag_send.at[way, step, slot], ag_recv.at[way, step, slot], targets[way])

    def fin_copy(idx, way):
        chunk = ag_chunk(way, 0)
        return pltpu.make_async_copy(acc_rows(idx, way, chunk), out_rows(idx, core, way, chunk),
                                     fin_sem.at[way, lax.rem(idx, MSG_SLOTS)])

    def peer_copy(idx, way, step):
        slot = lax.rem(idx, MSG_SLOTS)
        rows = out_rows(idx, core, way, ag_chunk(way, step))
        src = acc_rows(idx, way, ag_chunk(way, 0)) if step == 0 else rows
        return remote(src, rows, peer_send.at[way, step, slot], peer_recv.at[way, step, slot], partner)


    def post_copies(idx):
        slot = lax.rem(idx, 2)
        rows = quad_rows(lax.rem(idx, nquad))
        y_copy = pltpu.make_async_copy(wo_ref.at[rows], wbuf.at[slot, 1], w_sem.at[slot, 1])
        return [pltpu.make_async_copy(ref.at[rows], wbuf.at[slot, 0], w_sem.at[slot, 0]) for ref in (wq_ref, wv_ref, wk_ref)], y_copy

    def start_post(idx):
        dx_copies, y_copy = post_copies(idx)
        for kind in range(1, 4):
            @pl.when(idx // nquad == kind)
            def _():
                dx_copies[kind - 1].start()

        @pl.when(idx // nquad == 2)
        def _():
            y_copy.start()

    def accumulate(total, rows_t, weight, fresh):
        tile_t = 256

        def tile(step, carry):
            toks_at = pl.ds(pl.multiple_of(step * tile_t, tile_t), tile_t)
            add = mm(rows_t[:, toks_at], weight[...], TN)

            @pl.when(fresh)
            def _():
                total[toks_at, :] = add

            @pl.when(jnp.logical_not(fresh))
            def _():
                total[toks_at, :] += add
            return carry
        lax.fori_loop(0, toks // tile_t, tile, 0)

    def write_rows(total, dst):
        tile_t = row_out.shape[1]
        for i in range(toks // tile_t):
            copy = pltpu.make_async_copy(row_out.at[i % 2], dst.at[i * tile_t:(i + 1) * tile_t], row_sem.at[i % 2])
            if i >= 2:
                copy.wait()
            row_out[i % 2] = total[i * tile_t:(i + 1) * tile_t, :].astype(BF16)
            copy.start()
        for i in range(2):
            pltpu.make_async_copy(row_out.at[i], dst.at[i * tile_t:(i + 1) * tile_t], row_sem.at[i]).wait()

    def stage_post(idx):
        slot = lax.rem(idx, 2)
        kind = idx // nquad
        dx_copies, y_copy = post_copies(idx)
        dx_copies[0].wait()

        @pl.when(idx + 1 < count)
        def _():
            start_post(idx + 1)
        accumulate(dx_acc, lhs.at[slot], wbuf.at[slot, 0], idx == nquad)

        @pl.when(kind == 2)
        def _():
            y_copy.wait()
            accumulate(y_acc, ot.at[quad_rows(lax.rem(idx, nquad))], wbuf.at[slot, 1], idx == 2 * nquad)

        @pl.when(idx == 3 * nquad)
        def _():
            write_rows(y_acc, y_ref)

        @pl.when(idx == count - 1)
        def _():
            write_rows(dx_acc, dx_ref)

    def unit(idx, kind):
        quad = lax.rem(idx, nquad)
        slot = lax.rem(idx, 2)
        by_query = kind < 2
        left, right = (kt, qt) if kind % 2 == 0 else (vt, dt)
        value = (vt, kt, dt, qt)[kind]

        def head_step(head, carry):
            rows = pl.ds(pl.multiple_of(quad * QUAD + head * HEAD, HEAD), HEAD)
            for ob in range(nblk):
                total = None
                for ib in (range(ob + 1) if by_query else range(ob, nblk)):
                    tb, sb = (ob, ib) if by_query else (ib, ob)
                    t_cols, s_cols = pl.ds(tb * BLK, BLK), pl.ds(sb * BLK, BLK)
                    seen = row_id + float(sb * BLK) >= bound_ref[0:1, t_cols]
                    if sb == tb:
                        seen = jnp.logical_and(seen, diag)
                    prob = jnp.where(seen, mm(left[rows, s_cols], right[rows, t_cols], TN) * scale, 0.0).astype(BF16)
                    if by_query:
                        part_sum = mm(value[rows, s_cols], prob, NN)
                    else:
                        part_sum = mm(value[rows, t_cols], prob, NT)
                    total = part_sum if total is None else total + part_sum
                raw[pl.ds(pl.multiple_of(head * HEAD, HEAD), HEAD), ob * BLK:(ob + 1) * BLK] = total
            return carry

        lax.fori_loop(0, QUAD // HEAD, head_step, 0)
        state = s_in if by_query else r_in
        full = spread_states(state[pack_rows(quad), :]).astype(BF16)
        other = (qt, dt, kt, vt)[kind]
        dims = NN if kind % 2 == 0 else TN
        weight = jnp.where(bound < 0.0, scale, 0.0) if by_query else jnp.where(pos >= last_bound, scale, 0.0)
        for tb in range(nblk):
            cols = pl.ds(tb * BLK, BLK)
            extra = mm(full, other[quad_rows(quad), cols], dims) * weight[:, tb * BLK:(tb + 1) * BLK]
            lhs[slot, :, cols] = (raw[:, cols] + extra).astype(BF16)
            if kind == 0:
                ot[quad_rows(quad), cols] = lhs[slot, :, cols]

    def stage_partial(idx):
        slot = lax.rem(idx, 2)
        for kind in range(4):
            @pl.when(idx // nquad == kind)
            def _():
                unit(idx, kind)
        rhs_id = jnp.minimum(idx // nquad, 1)
        tile_n = 512 if width % 512 == 0 else width

        def tile(step, carry):
            cols = pl.ds(pl.multiple_of(step * tile_n, tile_n), tile_n)
            part[slot, :, cols] = mm(lhs[slot], xy[rhs_id, :, cols], NN)
            return carry
        lax.fori_loop(0, width // tile_n, tile, 0)
        pair_copy(idx).start()

        @pl.when(idx == nquad - 1)
        def _():
            start_post(idx + 1)

        @pl.when(idx >= nquad)
        def _():
            stage_post(idx)

    def add_rows(idx, way, step):
        chunk = sent_chunk(way, step)
        rows = pl.ds(pl.multiple_of(way * side + chunk * piece, piece), piece)
        slot = lax.rem(idx, ACC_SLOTS)
        acc[slot, rows, :] = acc[slot, rows, :] + inbox[way, step - 1, lax.rem(idx, MSG_SLOTS)]

    def stage_pair(idx):
        copy = pair_copy(idx)
        copy.wait()
        slot = lax.rem(idx, ACC_SLOTS)

        def add(step, carry):
            rows = pl.ds(pl.multiple_of(step * piece, piece), piece)
            own = pl.ds(pl.multiple_of(core * half + step * piece, piece), piece)
            acc[slot, rows, :] = acc[slot, rows, :] + part[lax.rem(idx, 2), own, :]
            return carry
        lax.fori_loop(0, half // piece, add, 0)
        for way in range(2):
            rs_copy(idx, way, 0).start()

    def stage_reduce(idx, step):
        for way in range(2):
            prev = rs_copy(idx, way, step - 1)
            prev.wait_send()
            prev.wait_recv()
            add_rows(idx, way, step)
            if step < chips - 1:
                rs_copy(idx, way, step).start()
            else:
                ag_copy(idx, way, 0).start()
                peer_copy(idx, way, 0).start()
                fin_copy(idx, way).start()

    def stage_gather(idx, step):
        for way in range(2):
            ag_copy(idx, way, step).wait_send()
            slot = lax.rem(idx, MSG_SLOTS)
            got = out_rows(idx, core, way, ag_chunk(way, step + 1))
            remote(got, got, ag_send.at[way, step, slot], ag_recv.at[way, step, slot], targets[way]).wait_recv()
            if step + 1 < chips - 1:
                ag_copy(idx, way, step + 1).start()
            peer_copy(idx, way, step + 1).start()
            if step == 0:
                fin_copy(idx, way).wait()
            finish_peer(idx, way, step)

    def finish_peer(idx, way, step):
        peer_copy(idx, way, step).wait_send()
        slot = lax.rem(idx, MSG_SLOTS)
        got = out_rows(idx, 1 - core, way, ag_chunk(way, step))
        remote(got, got, peer_send.at[way, step, slot], peer_recv.at[way, step, slot], partner).wait_recv()

    def stage_last(idx):
        for way in range(2):
            finish_peer(idx, way, chips - 1)

    order = [(2 * chips, stage_last)]
    for step in reversed(range(chips - 1)):
        order.append((chips + 1 + step, functools.partial(stage_gather, step=step)))
    for step in reversed(range(1, chips)):
        order.append((1 + step, functools.partial(stage_reduce, step=step)))
    order.append((1, stage_pair))
    order.append((0, stage_partial))
    lead = max(devs - 1, nquad)

    def tick_step(tick, carry):
        @pl.when(tick < nquad)
        def _():
            project_kv(tick)

        @pl.when(jnp.logical_and(tick >= nquad, tick < 2 * nquad))
        def _():
            project_qd(tick)
        s_quad = tick - me
        r_quad = tick - nquad - (devs - 1 - me)

        @pl.when(jnp.logical_and(s_quad >= 0, s_quad < nquad))
        def _():
            chain_step(0, s_quad, me == 0, me == devs - 1)

        @pl.when(jnp.logical_and(r_quad >= 0, r_quad < nquad))
        def _():
            chain_step(1, r_quad, me == devs - 1, me == 0)
        for delay, stage in order:
            idx = tick - lead - delay

            @pl.when(jnp.logical_and(idx >= 0, idx < count))
            def _():
                stage(idx)
        return carry

    lax.fori_loop(0, lead + count + 2 * chips, tick_step, 0)

    def chain_end(quad, carry):
        @pl.when(me < devs - 1)
        def _():
            chain_copy(0, quad).wait_send()

        @pl.when(me > 0)
        def _():
            chain_copy(1, quad).wait_send()
        return carry
    lax.fori_loop(0, nquad, chain_end, 0)


def fused(devs, scale, flags, x_loc, dy_loc, wq, wk, wv, wo):
    toks, width = x_loc.shape
    chips = devs // 2
    nquad = width // QUAD
    piece = QUAD // 4 // chips
    dma = pltpu.SemaphoreType.DMA
    act = jax.ShapeDtypeStruct((toks, width), BF16)
    state = pltpu.VMEM((width // 2, 2 * HEAD), F32)
    ring = (2, chips - 1, MSG_SLOTS)
    return pl.pallas_call(
        functools.partial(fused_kernel, devs, scale),
        name='fused',
        in_specs=[pl.BlockSpec(memory_space=pltpu.VMEM)] + [pl.BlockSpec(memory_space=pl.ANY)] * 6,
        out_specs=[pl.BlockSpec(memory_space=pl.ANY)] * 3,
        out_shape=[jax.ShapeDtypeStruct((4 * width, width), F32)] + [act] * 2,
        scratch_shapes=[
            pltpu.VMEM((2, toks, width), BF16),
            pltpu.VMEM((2, 2, QUAD, width), BF16),
            *[pltpu.VMEM((width, toks), BF16)] * 4,
            *[state] * 6,
            pltpu.VMEM((8, toks), F32),
            pltpu.VMEM((QUAD, toks), F32),
            pltpu.VMEM((2, QUAD, toks), BF16),
            pltpu.VMEM((width, toks), BF16),
            pltpu.VMEM((2, QUAD, width), F32),
            pltpu.VMEM((ACC_SLOTS, QUAD // 2, width), F32),
            pltpu.VMEM((2, chips - 1, MSG_SLOTS, piece, width), F32),
            pltpu.VMEM((toks, width), F32),
            pltpu.VMEM((toks, width), F32),
            pltpu.VMEM((2, 128, width), BF16),
            dma((2,)), dma((2, 2)), dma((2,)), dma((2, nquad)), dma((2, nquad)), dma((ACC_SLOTS,)), dma((ACC_SLOTS,)),
            dma(ring), dma(ring), dma(ring), dma(ring), dma((2, MSG_SLOTS)),
            dma((2, chips, MSG_SLOTS)), dma((2, chips, MSG_SLOTS)),
        ],
        compiler_params=pltpu.CompilerParams(vmem_limit_bytes=VMEM_CAP, collective_id=0, has_side_effects=True),
        cost_estimate=pl.CostEstimate(flops=24 * toks * width * width, bytes_accessed=150 * 1024 * 1024, transcendentals=0),
    )(flags.reshape(1, toks), x_loc, dy_loc, wq, wk, wv, wo)


def solution(mesh):
    devs = mesh.shape['sp']

    def device_body(x_loc, flag_loc, w_q, w_k, w_v, w_o, dy_loc):
        toks, width = x_loc.shape
        heads, head_dim = w_q.shape[1], w_q.shape[2]
        scale = 1.0 / (math.sqrt(head_dim) * toks)
        wq, wk, wv = [jnp.transpose(w, (1, 2, 0)).reshape(width, width) for w in (w_q, w_k, w_v)]
        wo = w_o.reshape(width, width)
        total, y_loc, dx_loc = fused(devs, scale, flag_loc, x_loc, dy_loc, wq, wk, wv, wo)
        dw_o, dw_q, dw_v, dw_k = [total[i * width:(i + 1) * width].reshape(heads, head_dim, width) for i in range(4)]
        dw_q, dw_k, dw_v = [jnp.transpose(dw, (2, 0, 1)) for dw in (dw_q, dw_k, dw_v)]
        return y_loc, dx_loc, dw_q, dw_k, dw_v, dw_o

    row_spec = P(('dp', 'sp'), None)
    flag_spec = P(('dp', 'sp'))
    w_spec = P(None, None, None)
    dw_spec = P('dp', None, None)
    return jax.shard_map(device_body, mesh=mesh,
                         in_specs=(row_spec, flag_spec, w_spec, w_spec, w_spec, w_spec, row_spec),
                         out_specs=(row_spec, row_spec, dw_spec, dw_spec, dw_spec, dw_spec),
                         check_vma=False)
```

```python
import functools
import math
import jax
import jax.numpy as jnp
from jax import lax
from jax.experimental import pallas as pl
from jax.experimental.pallas import tpu as pltpu
from jax.sharding import PartitionSpec as P

MESH = pl.DeviceIdType.MESH
BF16 = jnp.bfloat16
F32 = jnp.float32
HEAD = 64
QUAD = 4 * HEAD
BLK = 256
VMEM_CAP = 64 * 1024 * 1024 - 128 * 1024
ACC_SLOTS = 8
MSG_SLOTS = 4
FAST = 4

NN = (((1,), (0,)), ((), ()))
NT = (((1,), (1,)), ((), ()))
TN = (((0,), (0,)), ((), ()))


def mm(lhs, rhs, dims):
    return lax.dot_general(lhs, rhs, dims, preferred_element_type=F32)


def pack_states(full):
    lane = lax.broadcasted_iota(jnp.int32, (HEAD, 2 * HEAD), 1)
    first = jnp.where(lane < HEAD, full[0:HEAD, 0:2 * HEAD], full[HEAD:2 * HEAD, 0:2 * HEAD])
    second = jnp.where(lane < HEAD, full[2 * HEAD:3 * HEAD, 2 * HEAD:], full[3 * HEAD:, 2 * HEAD:])
    return jnp.concatenate([first, second], axis=0)


def spread_states(packed):
    lane = lax.broadcasted_iota(jnp.int32, (HEAD, 2 * HEAD), 1)
    zero = jnp.zeros((HEAD, 2 * HEAD), F32)
    rows = []
    for head in range(4):
        pair = packed[(head // 2) * HEAD:(head // 2 + 1) * HEAD, :]
        own = jnp.where((lane < HEAD) == (head % 2 == 0), pair, 0.0)
        rows.append(jnp.concatenate([own, zero] if head < 2 else [zero, own], axis=1))
    return jnp.concatenate(rows, axis=0)


def fused_kernel(devs, scale, flag_ref, x_ref, dy_ref, wq_ref, wk_ref, wv_ref, wo_ref,
                 out_ref, y_ref, dx_ref,
                 xy, wbuf, qt, kt, vt, dt, mt, pre_in, nt, s_got, s_in, r_in, s_out, r_out, bound_ref, raw, lhs, ot, part, acc, inbox, y_acc, dx_acc, row_out,
                 xy_sem, w_sem, row_sem, pre_send, pre_recv, side_send, chain_send, chain_recv, pair_send, pair_recv, rs_send, rs_recv,
                 ag_send, ag_recv, fin_sem, peer_send, peer_recv):
    width, toks = qt.shape
    nquad = width // QUAD
    nblk = toks // BLK
    seg = QUAD
    count = 4 * nquad
    chips = devs // 2
    half = seg // 2
    side = seg // 4
    piece = side // chips
    me = lax.axis_index('sp')
    core = lax.rem(me, 2)
    chip = me // 2
    partner = chip * 2 + 1 - core
    targets = (lax.rem(chip + 1, chips) * 2 + core, lax.rem(chip + chips - 1, chips) * 2 + core)
    down = lax.rem(me + devs - 1, devs)

    load_x = pltpu.make_async_copy(x_ref, xy.at[1], xy_sem.at[1])
    load_dy = pltpu.make_async_copy(dy_ref, xy.at[0], xy_sem.at[0])
    load_x.start()

    def w_copies(quad, kv):
        slot = lax.rem(quad, 2)
        pair, base = ((wk_ref, wv_ref), 0) if kv else ((wq_ref, wo_ref), 2)
        return [pltpu.make_async_copy(ref.at[pl.ds(pl.multiple_of(quad * QUAD, QUAD), QUAD)], wbuf.at[slot, base + i],
                                      w_sem.at[slot, base + i]) for i, ref in enumerate(pair)]

    def start_w(quad, kv):
        @pl.when(quad < nquad)
        def _():
            for copy in w_copies(quad, kv):
                copy.start()

    start_w(jnp.int32(0), True)
    start_w(jnp.int32(0), False)
    load_dy.start()

    barrier = pltpu.get_barrier_semaphore()
    cross = tuple(lax.rem(chip + hop, chips) * 2 + 1 - core for hop in (1, chips - 1))
    for dev in (partner,) + targets + cross:
        pl.semaphore_signal(barrier, inc=1, device_id={'sp': dev}, device_id_type=MESH)

    lane = lax.broadcasted_iota(jnp.int32, (8, toks), 1)
    last = jnp.where(jnp.broadcast_to(flag_ref[...], (8, toks)) > 0, lane.astype(F32), -1.0)
    step = 1
    while step < toks:
        last = jnp.maximum(last, jnp.where(lane >= step, pltpu.roll(last, step, 1), -1.0))
        step *= 2
    bound_ref[...] = last
    bound = bound_ref[0:1, :]
    last_bound = jnp.max(bound, axis=1, keepdims=True)
    pos = lax.broadcasted_iota(jnp.int32, (1, toks), 1).astype(F32)
    gate = jnp.where(last_bound < 0.0, 1.0, 0.0)
    diag = (lax.broadcasted_iota(jnp.int32, (BLK, BLK), 0) <= lax.broadcasted_iota(jnp.int32, (BLK, BLK), 1))
    row_id = lax.broadcasted_iota(jnp.int32, (BLK, BLK), 0).astype(F32)

    pl.semaphore_wait(barrier, 5)
    load_x.wait()

    def quad_rows(quad):
        return pl.ds(pl.multiple_of(quad * QUAD, QUAD), QUAD)

    def pack_rows(quad):
        return pl.ds(pl.multiple_of(quad * (QUAD // 2), QUAD // 2), QUAD // 2)

    def project_kv(quad):
        slot = lax.rem(quad, 2)
        for copy in w_copies(quad, True):
            copy.wait()
        start_w(quad + 1, True)
        x_val = xy[1]
        k_val = mm(wbuf[slot, 0], x_val, NT).astype(BF16)
        kt[quad_rows(quad), :] = k_val
        v_raw = mm(wbuf[slot, 1], x_val, NT)
        vt[quad_rows(quad), :] = v_raw.astype(BF16)
        tail = pos >= last_bound
        mt[quad, 0:QUAD // 2, :] = pack_states(mm(jnp.where(tail, v_raw, 0.0).astype(BF16), k_val, NT))
        mt[quad, QUAD // 2:, :] = jnp.broadcast_to(gate, (8, 2 * HEAD))

        @pl.when(core == 0)
        def _():
            pre_copy(quad).start()

    def project_qd(quad):
        slot = lax.rem(quad, 2)
        for copy in w_copies(quad, False):
            copy.wait()
        start_w(quad + 1, False)

        @pl.when(quad == 0)
        def _():
            load_dy.wait()
        q_val = mm(wbuf[slot, 2], xy[1], NT).astype(BF16)
        qt[quad_rows(quad), :] = q_val
        d_raw = mm(wbuf[slot, 3], xy[0], NT)
        dt[quad_rows(quad), :] = d_raw.astype(BF16)
        nt[pack_rows(quad), :] = pack_states(mm(jnp.where(bound < 0.0, d_raw, 0.0).astype(BF16), q_val, NT))

    def pre_copy(quad):
        return pltpu.make_async_remote_copy(src_ref=mt.at[quad], dst_ref=pre_in.at[quad], send_sem=pre_send.at[quad],
                                            recv_sem=pre_recv.at[quad], device_id={'sp': partner}, device_id_type=MESH)

    def state_copy(quad, same_core):
        rows = pack_rows(quad)
        base = lax.rem(chip + 1, chips) * 2
        dev, sem = (base + 1, chain_send.at[0, quad]) if same_core else (base, side_send.at[quad])
        return pltpu.make_async_remote_copy(src_ref=s_out.at[rows], dst_ref=s_got.at[rows], send_sem=sem,
                                            recv_sem=chain_recv.at[0, quad], device_id={'sp': dev}, device_id_type=MESH)

    def state_step(quad):
        rows = pack_rows(quad)

        @pl.when(chip == 0)
        def _():
            s_got[rows, :] = jnp.zeros((QUAD // 2, 2 * HEAD), F32)

        @pl.when(chip > 0)
        def _():
            state_copy(quad, True).wait_recv()

        @pl.when(core == 0)
        def _():
            s_in[rows, :] = s_got[rows, :]

        @pl.when(core == 1)
        def _():
            pre_copy(quad).wait_recv()
            mine = pre_in[quad, QUAD // 2:QUAD // 2 + 1, :] * s_got[rows, :] + pre_in[quad, 0:QUAD // 2, :]
            s_in[rows, :] = mine

            @pl.when(chip < chips - 1)
            def _():
                s_out[rows, :] = gate * mine + mt[quad, 0:QUAD // 2, :]
                state_copy(quad, True).start()
                state_copy(quad, False).start()

    def chain_copy(quad):
        rows = pack_rows(quad)
        return pltpu.make_async_remote_copy(src_ref=r_out.at[rows], dst_ref=r_in.at[rows], send_sem=chain_send.at[1, quad],
                                            recv_sem=chain_recv.at[1, quad], device_id={'sp': down}, device_id_type=MESH)

    def chain_step(quad):
        rows = pack_rows(quad)

        @pl.when(me == devs - 1)
        def _():
            r_in[rows, :] = jnp.zeros((QUAD // 2, 2 * HEAD), F32)

        @pl.when(me < devs - 1)
        def _():
            chain_copy(quad).wait_recv()

        @pl.when(me > 0)
        def _():
            r_out[rows, :] = gate * r_in[rows, :] + nt[rows, :]
            chain_copy(quad).start()

    def remote(src, dst, s_sem, r_sem, dev):
        return pltpu.make_async_remote_copy(src_ref=src, dst_ref=dst, send_sem=s_sem, recv_sem=r_sem,
                                            device_id={'sp': dev}, device_id_type=MESH)

    def ring_idx(idx):
        return lax.rem(idx + 4 * chips, chips)

    def pair_copy(idx):
        slot = lax.rem(idx, ACC_SLOTS)
        src = part.at[lax.rem(idx, 2), pl.ds(pl.multiple_of((1 - core) * half, half), half)]
        return remote(src, acc.at[slot], pair_send.at[slot], pair_recv.at[slot], partner)

    def acc_rows(idx, way, chunk):
        return acc.at[lax.rem(idx, ACC_SLOTS), pl.ds(pl.multiple_of(way * side + chunk * piece, piece), piece)]

    def out_rows(idx, owner, way, chunk):
        row = idx * seg + owner * half + way * side + chunk * piece
        return out_ref.at[pl.ds(pl.multiple_of(row, piece), piece)]

    def sent_chunk(way, step):
        return ring_idx(chip - step if way == 0 else chip + step)

    def rs_copy(idx, way, step):
        slot = lax.rem(idx, MSG_SLOTS)
        return remote(acc_rows(idx, way, sent_chunk(way, step)), inbox.at[way, step, slot],
                      rs_send.at[way, step, slot], rs_recv.at[way, step, slot], targets[way])

    def ag_chunk(way, step):
        return ring_idx(chip + 1 - step if way == 0 else chip - 1 + step)

    def ag_copy(idx, way, step):
        slot = lax.rem(idx, MSG_SLOTS)
        rows = out_rows(idx, core, way, ag_chunk(way, step))
        src = acc_rows(idx, way, ag_chunk(way, 0)) if step == 0 else rows
        return remote(src, rows, ag_send.at[way, step, slot], ag_recv.at[way, step, slot], targets[way])

    def fin_copy(idx, way):
        chunk = ag_chunk(way, 0)
        return pltpu.make_async_copy(acc_rows(idx, way, chunk), out_rows(idx, core, way, chunk),
                                     fin_sem.at[way, lax.rem(idx, MSG_SLOTS)])

    def peer_copy(idx, way, step):
        slot = lax.rem(idx, MSG_SLOTS)
        rows = out_rows(idx, core, way, ag_chunk(way, step))
        src = acc_rows(idx, way, ag_chunk(way, 0)) if step == 0 else rows
        return remote(src, rows, peer_send.at[way, step, slot], peer_recv.at[way, step, slot], partner)


    def post_copies(idx):
        slot = lax.rem(idx, 2)
        rows = quad_rows(lax.rem(idx, nquad))
        y_copy = pltpu.make_async_copy(wo_ref.at[rows], wbuf.at[slot, 1], w_sem.at[slot, 1])
        return [pltpu.make_async_copy(ref.at[rows], wbuf.at[slot, 0], w_sem.at[slot, 0]) for ref in (wq_ref, wv_ref, wk_ref)], y_copy

    def start_post(idx):
        dx_copies, y_copy = post_copies(idx)
        for kind in range(1, 4):
            @pl.when(idx // nquad == kind)
            def _():
                dx_copies[kind - 1].start()

        @pl.when(idx // nquad == 2)
        def _():
            y_copy.start()

    def accumulate(total, rows_t, weight, fresh):
        tile_t = 256

        def tile(step, carry):
            toks_at = pl.ds(pl.multiple_of(step * tile_t, tile_t), tile_t)
            add = mm(rows_t[:, toks_at], weight[...], TN)

            @pl.when(fresh)
            def _():
                total[toks_at, :] = add

            @pl.when(jnp.logical_not(fresh))
            def _():
                total[toks_at, :] += add
            return carry
        lax.fori_loop(0, toks // tile_t, tile, 0)

    def write_rows(total, dst):
        tile_t = row_out.shape[1]
        for i in range(toks // tile_t):
            copy = pltpu.make_async_copy(row_out.at[i % 2], dst.at[i * tile_t:(i + 1) * tile_t], row_sem.at[i % 2])
            if i >= 2:
                copy.wait()
            row_out[i % 2] = total[i * tile_t:(i + 1) * tile_t, :].astype(BF16)
            copy.start()
        for i in range(2):
            pltpu.make_async_copy(row_out.at[i], dst.at[i * tile_t:(i + 1) * tile_t], row_sem.at[i]).wait()

    def stage_post(idx):
        slot = lax.rem(idx, 2)
        kind = idx // nquad
        dx_copies, y_copy = post_copies(idx)
        dx_copies[0].wait()

        @pl.when(idx + 1 < count)
        def _():
            start_post(idx + 1)
        accumulate(dx_acc, lhs.at[slot], wbuf.at[slot, 0], idx == nquad)

        @pl.when(kind == 2)
        def _():
            y_copy.wait()
            accumulate(y_acc, ot.at[quad_rows(lax.rem(idx, nquad))], wbuf.at[slot, 1], idx == 2 * nquad)

        @pl.when(idx == 3 * nquad)
        def _():
            write_rows(y_acc, y_ref)

        @pl.when(idx == count - 1)
        def _():
            write_rows(dx_acc, dx_ref)

    def unit(idx, kind):
        quad = lax.rem(idx, nquad)
        slot = lax.rem(idx, 2)
        by_query = kind < 2
        left, right = (kt, qt) if kind % 2 == 0 else (vt, dt)
        value = (vt, kt, dt, qt)[kind]

        def head_step(head, carry):
            rows = pl.ds(pl.multiple_of(quad * QUAD + head * HEAD, HEAD), HEAD)
            for ob in range(nblk):
                total = None
                for ib in (range(ob + 1) if by_query else range(ob, nblk)):
                    tb, sb = (ob, ib) if by_query else (ib, ob)
                    t_cols, s_cols = pl.ds(tb * BLK, BLK), pl.ds(sb * BLK, BLK)
                    seen = row_id + float(sb * BLK) >= bound_ref[0:1, t_cols]
                    if sb == tb:
                        seen = jnp.logical_and(seen, diag)
                    prob = jnp.where(seen, mm(left[rows, s_cols], right[rows, t_cols], TN) * scale, 0.0).astype(BF16)
                    if by_query:
                        part_sum = mm(value[rows, s_cols], prob, NN)
                    else:
                        part_sum = mm(value[rows, t_cols], prob, NT)
                    total = part_sum if total is None else total + part_sum
                raw[pl.ds(pl.multiple_of(head * HEAD, HEAD), HEAD), ob * BLK:(ob + 1) * BLK] = total
            return carry

        lax.fori_loop(0, QUAD // HEAD, head_step, 0)
        state = s_in if by_query else r_in
        full = spread_states(state[pack_rows(quad), :]).astype(BF16)
        other = (qt, dt, kt, vt)[kind]
        dims = NN if kind % 2 == 0 else TN
        weight = jnp.where(bound < 0.0, scale, 0.0) if by_query else jnp.where(pos >= last_bound, scale, 0.0)
        for tb in range(nblk):
            cols = pl.ds(tb * BLK, BLK)
            extra = mm(full, other[quad_rows(quad), cols], dims) * weight[:, tb * BLK:(tb + 1) * BLK]
            lhs[slot, :, cols] = (raw[:, cols] + extra).astype(BF16)
            if kind == 0:
                ot[quad_rows(quad), cols] = lhs[slot, :, cols]

    def stage_unit(idx):
        for kind in range(4):
            @pl.when(idx // nquad == kind)
            def _():
                unit(idx, kind)

    def stage_partial(idx):
        slot = lax.rem(idx, 2)
        rhs_id = jnp.minimum(idx // nquad, 1)
        tile_n = 512 if width % 512 == 0 else width

        def tile(step, carry):
            cols = pl.ds(pl.multiple_of(step * tile_n, tile_n), tile_n)
            part[slot, :, cols] = mm(lhs[slot], xy[rhs_id, :, cols], NN)
            return carry
        lax.fori_loop(0, width // tile_n, tile, 0)
        pair_copy(idx).start()

        @pl.when(idx == nquad - 1)
        def _():
            start_post(idx + 1)

        @pl.when(idx >= nquad)
        def _():
            stage_post(idx)

    def add_rows(idx, way, step):
        chunk = sent_chunk(way, step)
        rows = pl.ds(pl.multiple_of(way * side + chunk * piece, piece), piece)
        slot = lax.rem(idx, ACC_SLOTS)
        acc[slot, rows, :] = acc[slot, rows, :] + inbox[way, step - 1, lax.rem(idx, MSG_SLOTS)]

    def stage_pair(idx):
        copy = pair_copy(idx)
        copy.wait()
        slot = lax.rem(idx, ACC_SLOTS)

        def add(step, carry):
            rows = pl.ds(pl.multiple_of(step * piece, piece), piece)
            own = pl.ds(pl.multiple_of(core * half + step * piece, piece), piece)
            acc[slot, rows, :] = acc[slot, rows, :] + part[lax.rem(idx, 2), own, :]
            return carry
        lax.fori_loop(0, half // piece, add, 0)
        for way in range(2):
            rs_copy(idx, way, 0).start()

    def stage_reduce(idx, step):
        for way in range(2):
            prev = rs_copy(idx, way, step - 1)
            prev.wait_send()
            prev.wait_recv()
            add_rows(idx, way, step)
            if step < chips - 1:
                rs_copy(idx, way, step).start()
            else:
                ag_copy(idx, way, 0).start()
                peer_copy(idx, way, 0).start()
                fin_copy(idx, way).start()

    def stage_gather(idx, step):
        for way in range(2):
            ag_copy(idx, way, step).wait_send()
            slot = lax.rem(idx, MSG_SLOTS)
            got = out_rows(idx, core, way, ag_chunk(way, step + 1))
            remote(got, got, ag_send.at[way, step, slot], ag_recv.at[way, step, slot], targets[way]).wait_recv()
            if step + 1 < chips - 1:
                ag_copy(idx, way, step + 1).start()
            peer_copy(idx, way, step + 1).start()
            if step == 0:
                fin_copy(idx, way).wait()
            finish_peer(idx, way, step)

    def finish_peer(idx, way, step):
        peer_copy(idx, way, step).wait_send()
        slot = lax.rem(idx, MSG_SLOTS)
        got = out_rows(idx, 1 - core, way, ag_chunk(way, step))
        remote(got, got, peer_send.at[way, step, slot], peer_recv.at[way, step, slot], partner).wait_recv()

    def stage_last(idx):
        for way in range(2):
            finish_peer(idx, way, chips - 1)

    order = [(2 * chips, stage_last)]
    for step in reversed(range(chips - 1)):
        order.append((chips + 1 + step, functools.partial(stage_gather, step=step)))
    for step in reversed(range(1, chips)):
        order.append((1 + step, functools.partial(stage_reduce, step=step)))
    order.append((1, stage_pair))
    lead = chips

    def when_in(idx, limit, body):
        @pl.when(jnp.logical_and(idx >= 0, idx < limit))
        def _():
            body(idx)

    def tick_step(tick, carry):
        when_in(tick, nquad, project_kv)
        when_in(tick - lead, nquad, project_qd)
        when_in(tick - 1 - chip, nquad, state_step)
        when_in(tick - lead - (devs - 1 - me), nquad, chain_step)
        rnd = tick - lead

        def poll(turn, carry):
            for delay, stage in order:
                slow = rnd - delay
                quick = rnd - (delay + 1) // 2
                on_turn = turn == (0 if delay % 2 else 1)
                is_quick = jnp.logical_and(on_turn, jnp.logical_and(quick >= 0, quick < FAST))
                is_slow = jnp.logical_and(turn == 0, jnp.logical_and(slow >= FAST, slow < count))

                @pl.when(jnp.logical_or(is_quick, is_slow))
                def _():
                    stage(jnp.where(is_quick, quick, slow))

            @pl.when(turn == 0)
            def _():
                when_in(rnd, count, stage_unit)

            @pl.when(turn == 1)
            def _():
                when_in(rnd, count, stage_partial)
            return carry
        lax.fori_loop(0, 2, poll, 0)
        return carry

    lax.fori_loop(0, lead + count + 2 * chips, tick_step, 0)

    def chain_end(quad, carry):
        @pl.when(core == 0)
        def _():
            pre_copy(quad).wait_send()

        @pl.when(jnp.logical_and(core == 1, chip < chips - 1))
        def _():
            state_copy(quad, True).wait_send()
            state_copy(quad, False).wait_send()

        @pl.when(me > 0)
        def _():
            chain_copy(quad).wait_send()
        return carry
    lax.fori_loop(0, nquad, chain_end, 0)


def fused(devs, scale, flags, x_loc, dy_loc, wq, wk, wv, wo):
    toks, width = x_loc.shape
    chips = devs // 2
    nquad = width // QUAD
    piece = QUAD // 4 // chips
    dma = pltpu.SemaphoreType.DMA
    act = jax.ShapeDtypeStruct((toks, width), BF16)
    state = pltpu.VMEM((width // 2, 2 * HEAD), F32)
    ring = (2, chips - 1, MSG_SLOTS)
    return pl.pallas_call(
        functools.partial(fused_kernel, devs, scale),
        name='fused',
        in_specs=[pl.BlockSpec(memory_space=pltpu.VMEM)] + [pl.BlockSpec(memory_space=pl.ANY)] * 6,
        out_specs=[pl.BlockSpec(memory_space=pl.ANY)] * 3,
        out_shape=[jax.ShapeDtypeStruct((4 * width, width), F32)] + [act] * 2,
        scratch_shapes=[
            pltpu.VMEM((2, toks, width), BF16),
            pltpu.VMEM((2, 4, QUAD, width), BF16),
            *[pltpu.VMEM((width, toks), BF16)] * 4,
            pltpu.VMEM((nquad, QUAD // 2 + 8, 2 * HEAD), F32),
            pltpu.VMEM((nquad, QUAD // 2 + 8, 2 * HEAD), F32),
            *[state] * 6,
            pltpu.VMEM((8, toks), F32),
            pltpu.VMEM((QUAD, toks), F32),
            pltpu.VMEM((2, QUAD, toks), BF16),
            pltpu.VMEM((width, toks), BF16),
            pltpu.VMEM((2, QUAD, width), F32),
            pltpu.VMEM((ACC_SLOTS, QUAD // 2, width), F32),
            pltpu.VMEM((2, chips - 1, MSG_SLOTS, piece, width), F32),
            pltpu.VMEM((toks, width), F32),
            pltpu.VMEM((toks, width), F32),
            pltpu.VMEM((2, 128, width), BF16),
            dma((2,)), dma((2, 4)), dma((2,)), dma((nquad,)), dma((nquad,)), dma((nquad,)), dma((2, nquad)), dma((2, nquad)), dma((ACC_SLOTS,)), dma((ACC_SLOTS,)),
            dma(ring), dma(ring), dma(ring), dma(ring), dma((2, MSG_SLOTS)),
            dma((2, chips, MSG_SLOTS)), dma((2, chips, MSG_SLOTS)),
        ],
        compiler_params=pltpu.CompilerParams(vmem_limit_bytes=VMEM_CAP, collective_id=0, has_side_effects=True),
        cost_estimate=pl.CostEstimate(flops=24 * toks * width * width, bytes_accessed=150 * 1024 * 1024, transcendentals=0),
    )(flags.reshape(1, toks), x_loc, dy_loc, wq, wk, wv, wo)


def solution(mesh):
    devs = mesh.shape['sp']

    def device_body(x_loc, flag_loc, w_q, w_k, w_v, w_o, dy_loc):
        toks, width = x_loc.shape
        heads, head_dim = w_q.shape[1], w_q.shape[2]
        scale = 1.0 / (math.sqrt(head_dim) * toks)
        wq, wk, wv = [jnp.transpose(w, (1, 2, 0)).reshape(width, width) for w in (w_q, w_k, w_v)]
        wo = w_o.reshape(width, width)
        total, y_loc, dx_loc = fused(devs, scale, flag_loc, x_loc, dy_loc, wq, wk, wv, wo)
        dw_o, dw_q, dw_v, dw_k = [total[i * width:(i + 1) * width].reshape(heads, head_dim, width) for i in range(4)]
        dw_q, dw_k, dw_v = [jnp.transpose(dw, (2, 0, 1)) for dw in (dw_q, dw_k, dw_v)]
        return y_loc, dx_loc, dw_q, dw_k, dw_v, dw_o

    row_spec = P(('dp', 'sp'), None)
    flag_spec = P(('dp', 'sp'))
    w_spec = P(None, None, None)
    dw_spec = P('dp', None, None)
    return jax.shard_map(device_body, mesh=mesh,
                         in_specs=(row_spec, flag_spec, w_spec, w_spec, w_spec, w_spec, row_spec),
                         out_specs=(row_spec, row_spec, dw_spec, dw_spec, dw_spec, dw_spec),
                         check_vma=False)
```

```python
import functools
import math
import jax
import jax.numpy as jnp
from jax import lax
from jax.experimental import pallas as pl
from jax.experimental.pallas import tpu as pltpu
from jax.sharding import PartitionSpec as P

MESH = pl.DeviceIdType.MESH
BF16 = jnp.bfloat16
F32 = jnp.float32
HEAD = 64
QUAD = 4 * HEAD
BLK = 256
VMEM_CAP = 64 * 1024 * 1024 - 128 * 1024
ACC_SLOTS = 8
MSG_SLOTS = 4
FAST = 4
LATE = 3

NN = (((1,), (0,)), ((), ()))
NT = (((1,), (1,)), ((), ()))
TN = (((0,), (0,)), ((), ()))


def mm(lhs, rhs, dims):
    return lax.dot_general(lhs, rhs, dims, preferred_element_type=F32)


def pack_states(full):
    lane = lax.broadcasted_iota(jnp.int32, (HEAD, 2 * HEAD), 1)
    first = jnp.where(lane < HEAD, full[0:HEAD, 0:2 * HEAD], full[HEAD:2 * HEAD, 0:2 * HEAD])
    second = jnp.where(lane < HEAD, full[2 * HEAD:3 * HEAD, 2 * HEAD:], full[3 * HEAD:, 2 * HEAD:])
    return jnp.concatenate([first, second], axis=0)


def spread_states(packed):
    lane = lax.broadcasted_iota(jnp.int32, (HEAD, 2 * HEAD), 1)
    zero = jnp.zeros((HEAD, 2 * HEAD), F32)
    rows = []
    for head in range(4):
        pair = packed[(head // 2) * HEAD:(head // 2 + 1) * HEAD, :]
        own = jnp.where((lane < HEAD) == (head % 2 == 0), pair, 0.0)
        rows.append(jnp.concatenate([own, zero] if head < 2 else [zero, own], axis=1))
    return jnp.concatenate(rows, axis=0)


def fused_kernel(devs, scale, flag_ref, x_ref, dy_ref, wq_ref, wk_ref, wv_ref, wo_ref,
                 out_ref, y_ref, dx_ref,
                 xy, wbuf, qt, kt, vt, dt, mt, pre_in, nt, s_got, s_in, r_in, s_out, r_out, bound_ref, raw, lhs, ot, part, acc, inbox, y_acc, dx_acc, row_out,
                 xy_sem, w_sem, row_sem, pre_send, pre_recv, side_send, chain_send, chain_recv, pair_send, pair_recv, rs_send, rs_recv,
                 ag_send, ag_recv, fin_sem, peer_send, peer_recv):
    width, toks = qt.shape
    nquad = width // QUAD
    nblk = toks // BLK
    seg = QUAD
    count = 4 * nquad
    chips = devs // 2
    half = seg // 2
    side = seg // 4
    piece = side // chips
    me = lax.axis_index('sp')
    core = lax.rem(me, 2)
    chip = me // 2
    partner = chip * 2 + 1 - core
    targets = (lax.rem(chip + 1, chips) * 2 + core, lax.rem(chip + chips - 1, chips) * 2 + core)
    down = lax.rem(me + devs - 1, devs)

    load_x = pltpu.make_async_copy(x_ref, xy.at[1], xy_sem.at[1])
    load_dy = pltpu.make_async_copy(dy_ref, xy.at[0], xy_sem.at[0])
    load_x.start()

    weights = (wk_ref, wv_ref, wq_ref, wo_ref)

    def w_copy(quad, which):
        slot = lax.rem(quad, 2)
        return pltpu.make_async_copy(weights[which].at[pl.ds(pl.multiple_of(quad * QUAD, QUAD), QUAD)], wbuf.at[slot, which],
                                     w_sem.at[slot, which])

    def start_w(quad, which):
        @pl.when(quad < nquad)
        def _():
            w_copy(quad, which).start()

    start_w(jnp.int32(0), 0)
    start_w(jnp.int32(0), 1)
    start_w(jnp.int32(0), 2)
    start_w(jnp.int32(0), 3)
    load_dy.start()

    barrier = pltpu.get_barrier_semaphore()
    cross = tuple(lax.rem(chip + hop, chips) * 2 + 1 - core for hop in (1, chips - 1))
    for dev in (partner,) + targets + cross:
        pl.semaphore_signal(barrier, inc=1, device_id={'sp': dev}, device_id_type=MESH)

    lane = lax.broadcasted_iota(jnp.int32, (8, toks), 1)
    last = jnp.where(jnp.broadcast_to(flag_ref[...], (8, toks)) > 0, lane.astype(F32), -1.0)
    step = 1
    while step < toks:
        last = jnp.maximum(last, jnp.where(lane >= step, pltpu.roll(last, step, 1), -1.0))
        step *= 2
    bound_ref[...] = last
    bound = bound_ref[0:1, :]
    last_bound = jnp.max(bound, axis=1, keepdims=True)
    pos = lax.broadcasted_iota(jnp.int32, (1, toks), 1).astype(F32)
    gate = jnp.where(last_bound < 0.0, 1.0, 0.0)
    diag = (lax.broadcasted_iota(jnp.int32, (BLK, BLK), 0) <= lax.broadcasted_iota(jnp.int32, (BLK, BLK), 1))
    row_id = lax.broadcasted_iota(jnp.int32, (BLK, BLK), 0).astype(F32)

    pl.semaphore_wait(barrier, 5)
    load_x.wait()

    def quad_rows(quad):
        return pl.ds(pl.multiple_of(quad * QUAD, QUAD), QUAD)

    def pack_rows(quad):
        return pl.ds(pl.multiple_of(quad * (QUAD // 2), QUAD // 2), QUAD // 2)

    def project_kv(quad):
        slot = lax.rem(quad, 2)
        for which in range(2):
            w_copy(quad, which).wait()
            start_w(quad + 1, which)
        x_val = xy[1]
        k_val = mm(wbuf[slot, 0], x_val, NT).astype(BF16)
        kt[quad_rows(quad), :] = k_val
        v_raw = mm(wbuf[slot, 1], x_val, NT)
        vt[quad_rows(quad), :] = v_raw.astype(BF16)
        tail = pos >= last_bound
        mt[quad, 0:QUAD // 2, :] = pack_states(mm(jnp.where(tail, v_raw, 0.0).astype(BF16), k_val, NT))
        mt[quad, QUAD // 2:, :] = jnp.broadcast_to(gate, (8, 2 * HEAD))

        @pl.when(core == 0)
        def _():
            pre_copy(quad).start()

    def project_q(quad):
        w_copy(quad, 2).wait()
        start_w(quad + 1, 2)
        qt[quad_rows(quad), :] = mm(wbuf[lax.rem(quad, 2), 2], xy[1], NT).astype(BF16)

    def project_d(quad):
        w_copy(quad, 3).wait()
        start_w(quad + 1, 3)
        d_raw = mm(wbuf[lax.rem(quad, 2), 3], xy[0], NT)
        dt[quad_rows(quad), :] = d_raw.astype(BF16)
        nt[pack_rows(quad), :] = pack_states(mm(jnp.where(bound < 0.0, d_raw, 0.0).astype(BF16), qt[quad_rows(quad), :], NT))

    def pre_copy(quad):
        return pltpu.make_async_remote_copy(src_ref=mt.at[quad], dst_ref=pre_in.at[quad], send_sem=pre_send.at[quad],
                                            recv_sem=pre_recv.at[quad], device_id={'sp': partner}, device_id_type=MESH)

    def state_copy(quad, same_core):
        rows = pack_rows(quad)
        base = lax.rem(chip + 1, chips) * 2
        dev, sem = (base + 1, chain_send.at[0, quad]) if same_core else (base, side_send.at[quad])
        return pltpu.make_async_remote_copy(src_ref=s_out.at[rows], dst_ref=s_got.at[rows], send_sem=sem,
                                            recv_sem=chain_recv.at[0, quad], device_id={'sp': dev}, device_id_type=MESH)

    def state_step(quad):
        rows = pack_rows(quad)

        @pl.when(chip == 0)
        def _():
            s_got[rows, :] = jnp.zeros((QUAD // 2, 2 * HEAD), F32)

        @pl.when(chip > 0)
        def _():
            state_copy(quad, True).wait_recv()

        @pl.when(core == 0)
        def _():
            s_in[rows, :] = s_got[rows, :]

        @pl.when(core == 1)
        def _():
            pre_copy(quad).wait_recv()
            mine = pre_in[quad, QUAD // 2:QUAD // 2 + 1, :] * s_got[rows, :] + pre_in[quad, 0:QUAD // 2, :]
            s_in[rows, :] = mine

            @pl.when(chip < chips - 1)
            def _():
                s_out[rows, :] = gate * mine + mt[quad, 0:QUAD // 2, :]
                state_copy(quad, True).start()
                state_copy(quad, False).start()

    def chain_copy(quad):
        rows = pack_rows(quad)
        return pltpu.make_async_remote_copy(src_ref=r_out.at[rows], dst_ref=r_in.at[rows], send_sem=chain_send.at[1, quad],
                                            recv_sem=chain_recv.at[1, quad], device_id={'sp': down}, device_id_type=MESH)

    def chain_step(quad):
        rows = pack_rows(quad)

        @pl.when(me == devs - 1)
        def _():
            r_in[rows, :] = jnp.zeros((QUAD // 2, 2 * HEAD), F32)

        @pl.when(me < devs - 1)
        def _():
            chain_copy(quad).wait_recv()

        @pl.when(me > 0)
        def _():
            r_out[rows, :] = gate * r_in[rows, :] + nt[rows, :]
            chain_copy(quad).start()

    def remote(src, dst, s_sem, r_sem, dev):
        return pltpu.make_async_remote_copy(src_ref=src, dst_ref=dst, send_sem=s_sem, recv_sem=r_sem,
                                            device_id={'sp': dev}, device_id_type=MESH)

    def ring_idx(idx):
        return lax.rem(idx + 4 * chips, chips)

    def pair_copy(idx):
        slot = lax.rem(idx, ACC_SLOTS)
        src = part.at[lax.rem(idx, 2), pl.ds(pl.multiple_of((1 - core) * half, half), half)]
        return remote(src, acc.at[slot], pair_send.at[slot], pair_recv.at[slot], partner)

    def acc_rows(idx, way, chunk):
        return acc.at[lax.rem(idx, ACC_SLOTS), pl.ds(pl.multiple_of(way * side + chunk * piece, piece), piece)]

    def out_rows(idx, owner, way, chunk):
        row = idx * seg + owner * half + way * side + chunk * piece
        return out_ref.at[pl.ds(pl.multiple_of(row, piece), piece)]

    def sent_chunk(way, step):
        return ring_idx(chip - step if way == 0 else chip + step)

    def rs_copy(idx, way, step):
        slot = lax.rem(idx, MSG_SLOTS)
        return remote(acc_rows(idx, way, sent_chunk(way, step)), inbox.at[way, step, slot],
                      rs_send.at[way, step, slot], rs_recv.at[way, step, slot], targets[way])

    def ag_chunk(way, step):
        return ring_idx(chip + 1 - step if way == 0 else chip - 1 + step)

    def ag_copy(idx, way, step):
        slot = lax.rem(idx, MSG_SLOTS)
        rows = out_rows(idx, core, way, ag_chunk(way, step))
        src = acc_rows(idx, way, ag_chunk(way, 0)) if step == 0 else rows
        return remote(src, rows, ag_send.at[way, step, slot], ag_recv.at[way, step, slot], targets[way])

    def fin_copy(idx, way):
        chunk = ag_chunk(way, 0)
        return pltpu.make_async_copy(acc_rows(idx, way, chunk), out_rows(idx, core, way, chunk),
                                     fin_sem.at[way, lax.rem(idx, MSG_SLOTS)])

    def peer_copy(idx, way, step):
        slot = lax.rem(idx, MSG_SLOTS)
        rows = out_rows(idx, core, way, ag_chunk(way, step))
        src = acc_rows(idx, way, ag_chunk(way, 0)) if step == 0 else rows
        return remote(src, rows, peer_send.at[way, step, slot], peer_recv.at[way, step, slot], partner)


    def post_copies(idx):
        slot = lax.rem(idx, 2)
        rows = quad_rows(lax.rem(idx, nquad))
        return [pltpu.make_async_copy(ref.at[rows], wbuf.at[slot, 0], w_sem.at[slot, 0]) for ref in (wq_ref, wv_ref, wk_ref)]

    def start_post(idx):
        for kind in range(1, 4):
            @pl.when(idx // nquad == kind)
            def _():
                post_copies(idx)[kind - 1].start()

    def y_copies(idx):
        slot = lax.rem(idx, 2)
        return [pltpu.make_async_copy(wo_ref.at[quad_rows(2 * idx + i)], wbuf.at[slot, 2 + i], w_sem.at[slot, 2 + i]) for i in range(2)]

    def stage_y(idx):
        for copy in y_copies(idx):
            copy.wait()

        @pl.when(idx + 1 < nquad // 2)
        def _():
            for copy in y_copies(idx + 1):
                copy.start()
        accumulate(y_acc, [(ot.at[quad_rows(2 * idx + i)], wbuf.at[lax.rem(idx, 2), 2 + i]) for i in range(2)], idx == 0)

        @pl.when(idx == nquad // 2 - 1)
        def _():
            write_rows(y_acc, y_ref)

    def accumulate(total, terms, fresh):
        tile_t = 128

        def tile(step, carry):
            toks_at = pl.ds(pl.multiple_of(step * tile_t, tile_t), tile_t)
            add = mm(terms[0][0][:, toks_at], terms[0][1][...], TN) + mm(terms[1][0][:, toks_at], terms[1][1][...], TN)

            @pl.when(fresh)
            def _():
                total[toks_at, :] = add

            @pl.when(jnp.logical_not(fresh))
            def _():
                total[toks_at, :] += add
            return carry
        lax.fori_loop(0, toks // tile_t, tile, 0)

    def write_rows(total, dst):
        tile_t = row_out.shape[1]
        for i in range(toks // tile_t):
            copy = pltpu.make_async_copy(row_out.at[i % 2], dst.at[i * tile_t:(i + 1) * tile_t], row_sem.at[i % 2])
            if i >= 2:
                copy.wait()
            row_out[i % 2] = total[i * tile_t:(i + 1) * tile_t, :].astype(BF16)
            copy.start()
        for i in range(2):
            pltpu.make_async_copy(row_out.at[i], dst.at[i * tile_t:(i + 1) * tile_t], row_sem.at[i]).wait()

    def stage_post(idx):
        post_copies(idx)[0].wait()

        @pl.when(lax.rem(idx, 2) == 1)
        def _():
            accumulate(dx_acc, [(lhs.at[slot], wbuf.at[slot, 0]) for slot in range(2)], idx == nquad + 1)

        @pl.when(idx + 1 < count)
        def _():
            start_post(idx + 1)

        @pl.when(idx == count - 1)
        def _():
            for copy in y_copies(jnp.int32(0)):
                copy.start()
            write_rows(dx_acc, dx_ref)

    def unit(idx, kind):
        quad = lax.rem(idx, nquad)
        slot = lax.rem(idx, 2)
        by_query = kind < 2
        left, right = (kt, qt) if kind % 2 == 0 else (vt, dt)
        value = (vt, kt, dt, qt)[kind]

        def head_step(head, carry):
            rows = pl.ds(pl.multiple_of(quad * QUAD + head * HEAD, HEAD), HEAD)
            for ob in range(nblk):
                total = None
                for ib in (range(ob + 1) if by_query else range(ob, nblk)):
                    tb, sb = (ob, ib) if by_query else (ib, ob)
                    t_cols, s_cols = pl.ds(tb * BLK, BLK), pl.ds(sb * BLK, BLK)
                    seen = row_id + float(sb * BLK) >= bound_ref[0:1, t_cols]
                    if sb == tb:
                        seen = jnp.logical_and(seen, diag)
                    prob = jnp.where(seen, mm(left[rows, s_cols], right[rows, t_cols], TN) * scale, 0.0).astype(BF16)
                    if by_query:
                        part_sum = mm(value[rows, s_cols], prob, NN)
                    else:
                        part_sum = mm(value[rows, t_cols], prob, NT)
                    total = part_sum if total is None else total + part_sum
                raw[pl.ds(pl.multiple_of(head * HEAD, HEAD), HEAD), ob * BLK:(ob + 1) * BLK] = total
            return carry

        lax.fori_loop(0, QUAD // HEAD, head_step, 0)
        state = s_in if by_query else r_in
        full = spread_states(state[pack_rows(quad), :]).astype(BF16)
        other = (qt, dt, kt, vt)[kind]
        dims = NN if kind % 2 == 0 else TN
        weight = jnp.where(bound < 0.0, scale, 0.0) if by_query else jnp.where(pos >= last_bound, scale, 0.0)
        for tb in range(nblk):
            cols = pl.ds(tb * BLK, BLK)
            extra = mm(full, other[quad_rows(quad), cols], dims) * weight[:, tb * BLK:(tb + 1) * BLK]
            lhs[slot, :, cols] = (raw[:, cols] + extra).astype(BF16)
            if kind == 0:
                ot[quad_rows(quad), cols] = lhs[slot, :, cols]

    def stage_unit(idx):
        for kind in range(4):
            @pl.when(idx // nquad == kind)
            def _():
                unit(idx, kind)

    def stage_partial(idx):
        slot = lax.rem(idx, 2)

        @pl.when(idx == 0)
        def _():
            load_dy.wait()
        rhs_id = jnp.minimum(idx // nquad, 1)
        tile_n = width // 2

        def tile(step, carry):
            cols = pl.ds(pl.multiple_of(step * tile_n, tile_n), tile_n)
            part[slot, :, cols] = mm(lhs[slot], xy[rhs_id, :, cols], NN)
            return carry
        lax.fori_loop(0, width // tile_n, tile, 0)
        pair_copy(idx).start()

        @pl.when(idx == nquad - 1)
        def _():
            start_post(idx + 1)

        @pl.when(idx >= nquad)
        def _():
            stage_post(idx)

    def add_rows(idx, way, step):
        chunk = sent_chunk(way, step)
        rows = pl.ds(pl.multiple_of(way * side + chunk * piece, piece), piece)
        slot = lax.rem(idx, ACC_SLOTS)
        acc[slot, rows, :] = acc[slot, rows, :] + inbox[way, step - 1, lax.rem(idx, MSG_SLOTS)]

    def stage_pair(idx):
        copy = pair_copy(idx)
        copy.wait()
        slot = lax.rem(idx, ACC_SLOTS)

        def add(step, carry):
            rows = pl.ds(pl.multiple_of(step * piece, piece), piece)
            own = pl.ds(pl.multiple_of(core * half + step * piece, piece), piece)
            acc[slot, rows, :] = acc[slot, rows, :] + part[lax.rem(idx, 2), own, :]
            return carry
        lax.fori_loop(0, half // piece, add, 0)
        for way in range(2):
            rs_copy(idx, way, 0).start()

    def stage_reduce(idx, step):
        for way in range(2):
            prev = rs_copy(idx, way, step - 1)
            prev.wait_send()
            prev.wait_recv()
            add_rows(idx, way, step)
            if step < chips - 1:
                rs_copy(idx, way, step).start()
            else:
                ag_copy(idx, way, 0).start()
                peer_copy(idx, way, 0).start()
                fin_copy(idx, way).start()

    def stage_gather(idx, step):
        for way in range(2):
            ag_copy(idx, way, step).wait_send()
            slot = lax.rem(idx, MSG_SLOTS)
            got = out_rows(idx, core, way, ag_chunk(way, step + 1))
            remote(got, got, ag_send.at[way, step, slot], ag_recv.at[way, step, slot], targets[way]).wait_recv()
            if step + 1 < chips - 1:
                ag_copy(idx, way, step + 1).start()
            peer_copy(idx, way, step + 1).start()
            if step == 0:
                fin_copy(idx, way).wait()
            finish_peer(idx, way, step)

    def finish_peer(idx, way, step):
        peer_copy(idx, way, step).wait_send()
        slot = lax.rem(idx, MSG_SLOTS)
        got = out_rows(idx, 1 - core, way, ag_chunk(way, step))
        remote(got, got, peer_send.at[way, step, slot], peer_recv.at[way, step, slot], partner).wait_recv()

    def stage_last(idx):
        for way in range(2):
            finish_peer(idx, way, chips - 1)

    order = [(2 * chips, stage_last)]
    for step in reversed(range(chips - 1)):
        order.append((chips + 1 + step, functools.partial(stage_gather, step=step)))
    for step in reversed(range(1, chips)):
        order.append((1 + step, functools.partial(stage_reduce, step=step)))
    order.append((1, stage_pair))
    lead = chips

    def when_in(idx, limit, body):
        @pl.when(jnp.logical_and(idx >= 0, idx < limit))
        def _():
            body(idx)

    def tick_step(tick, carry):
        when_in(tick, nquad, project_kv)
        when_in(tick - lead, nquad, project_q)
        when_in(tick - lead - LATE, nquad, project_d)
        when_in(tick - 1 - chip, nquad, state_step)
        when_in(tick - lead - LATE - (devs - 1 - me), nquad, chain_step)
        rnd = tick - lead

        def poll(turn, carry):
            for delay, stage in order:
                slow = rnd - delay
                quick = rnd - (delay + 1) // 2
                on_turn = turn == (0 if delay % 2 else 1)
                is_quick = jnp.logical_and(on_turn, jnp.logical_and(quick >= 0, quick < FAST))
                is_slow = jnp.logical_and(turn == 0, jnp.logical_and(slow >= FAST, slow < count))

                @pl.when(jnp.logical_or(is_quick, is_slow))
                def _():
                    stage(jnp.where(is_quick, quick, slow))

            @pl.when(turn == 0)
            def _():
                when_in(rnd, count, stage_unit)

            @pl.when(turn == 1)
            def _():
                when_in(rnd, count, stage_partial)
                when_in(rnd - count, nquad // 2, stage_y)
            return carry
        lax.fori_loop(0, 2, poll, 0)
        return carry

    lax.fori_loop(0, lead + count + 2 * chips, tick_step, 0)

    def chain_end(quad, carry):
        @pl.when(core == 0)
        def _():
            pre_copy(quad).wait_send()

        @pl.when(jnp.logical_and(core == 1, chip < chips - 1))
        def _():
            state_copy(quad, True).wait_send()
            state_copy(quad, False).wait_send()

        @pl.when(me > 0)
        def _():
            chain_copy(quad).wait_send()
        return carry
    lax.fori_loop(0, nquad, chain_end, 0)


def fused(devs, scale, flags, x_loc, dy_loc, wq, wk, wv, wo):
    toks, width = x_loc.shape
    chips = devs // 2
    nquad = width // QUAD
    piece = QUAD // 4 // chips
    dma = pltpu.SemaphoreType.DMA
    act = jax.ShapeDtypeStruct((toks, width), BF16)
    state = pltpu.VMEM((width // 2, 2 * HEAD), F32)
    ring = (2, chips - 1, MSG_SLOTS)
    return pl.pallas_call(
        functools.partial(fused_kernel, devs, scale),
        name='fused',
        in_specs=[pl.BlockSpec(memory_space=pltpu.VMEM)] + [pl.BlockSpec(memory_space=pl.ANY)] * 6,
        out_specs=[pl.BlockSpec(memory_space=pl.ANY)] * 3,
        out_shape=[jax.ShapeDtypeStruct((4 * width, width), F32)] + [act] * 2,
        scratch_shapes=[
            pltpu.VMEM((2, toks, width), BF16),
            pltpu.VMEM((2, 4, QUAD, width), BF16),
            *[pltpu.VMEM((width, toks), BF16)] * 4,
            pltpu.VMEM((nquad, QUAD // 2 + 8, 2 * HEAD), F32),
            pltpu.VMEM((nquad, QUAD // 2 + 8, 2 * HEAD), F32),
            *[state] * 6,
            pltpu.VMEM((8, toks), F32),
            pltpu.VMEM((QUAD, toks), F32),
            pltpu.VMEM((2, QUAD, toks), BF16),
            pltpu.VMEM((width, toks), BF16),
            pltpu.VMEM((2, QUAD, width), F32),
            pltpu.VMEM((ACC_SLOTS, QUAD // 2, width), F32),
            pltpu.VMEM((2, chips - 1, MSG_SLOTS, piece, width), F32),
            pltpu.VMEM((toks, width), F32),
            pltpu.VMEM((toks, width), F32),
            pltpu.VMEM((2, 128, width), BF16),
            dma((2,)), dma((2, 4)), dma((2,)), dma((nquad,)), dma((nquad,)), dma((nquad,)), dma((2, nquad)), dma((2, nquad)), dma((ACC_SLOTS,)), dma((ACC_SLOTS,)),
            dma(ring), dma(ring), dma(ring), dma(ring), dma((2, MSG_SLOTS)),
            dma((2, chips, MSG_SLOTS)), dma((2, chips, MSG_SLOTS)),
        ],
        compiler_params=pltpu.CompilerParams(vmem_limit_bytes=VMEM_CAP, collective_id=0, has_side_effects=True),
        cost_estimate=pl.CostEstimate(flops=24 * toks * width * width, bytes_accessed=150 * 1024 * 1024, transcendentals=0),
    )(flags.reshape(1, toks), x_loc, dy_loc, wq, wk, wv, wo)


def solution(mesh):
    devs = mesh.shape['sp']

    def device_body(x_loc, flag_loc, w_q, w_k, w_v, w_o, dy_loc):
        toks, width = x_loc.shape
        heads, head_dim = w_q.shape[1], w_q.shape[2]
        scale = 1.0 / (math.sqrt(head_dim) * toks)
        wq, wk, wv = [jnp.transpose(w, (1, 2, 0)).reshape(width, width) for w in (w_q, w_k, w_v)]
        wo = w_o.reshape(width, width)
        total, y_loc, dx_loc = fused(devs, scale, flag_loc, x_loc, dy_loc, wq, wk, wv, wo)
        dw_o, dw_q, dw_v, dw_k = [total[i * width:(i + 1) * width].reshape(heads, head_dim, width) for i in range(4)]
        dw_q, dw_k, dw_v = [jnp.transpose(dw, (2, 0, 1)) for dw in (dw_q, dw_k, dw_v)]
        return y_loc, dx_loc, dw_q, dw_k, dw_v, dw_o

    row_spec = P(('dp', 'sp'), None)
    flag_spec = P(('dp', 'sp'))
    w_spec = P(None, None, None)
    dw_spec = P('dp', None, None)
    return jax.shard_map(device_body, mesh=mesh,
                         in_specs=(row_spec, flag_spec, w_spec, w_spec, w_spec, w_spec, row_spec),
                         out_specs=(row_spec, row_spec, dw_spec, dw_spec, dw_spec, dw_spec),
                         check_vma=False)
```

```python
import functools
import math
import jax
import jax.numpy as jnp
from jax import lax
from jax.experimental import pallas as pl
from jax.experimental.pallas import tpu as pltpu
from jax.sharding import PartitionSpec as P

MESH = pl.DeviceIdType.MESH
BF16 = jnp.bfloat16
F32 = jnp.float32
HEAD = 64
QUAD = 4 * HEAD
BLK = 256
VMEM_CAP = 64 * 1024 * 1024 - 128 * 1024
ACC_SLOTS = 8
MSG_SLOTS = 4
FAST = 4
LATE = 3

NN = (((1,), (0,)), ((), ()))
NT = (((1,), (1,)), ((), ()))
TN = (((0,), (0,)), ((), ()))


def mm(lhs, rhs, dims):
    return lax.dot_general(lhs, rhs, dims, preferred_element_type=F32)


def pack_states(full):
    lane = lax.broadcasted_iota(jnp.int32, (HEAD, 2 * HEAD), 1)
    first = jnp.where(lane < HEAD, full[0:HEAD, 0:2 * HEAD], full[HEAD:2 * HEAD, 0:2 * HEAD])
    second = jnp.where(lane < HEAD, full[2 * HEAD:3 * HEAD, 2 * HEAD:], full[3 * HEAD:, 2 * HEAD:])
    return jnp.concatenate([first, second], axis=0)


def spread_states(packed):
    lane = lax.broadcasted_iota(jnp.int32, (HEAD, 2 * HEAD), 1)
    zero = jnp.zeros((HEAD, 2 * HEAD), F32)
    rows = []
    for head in range(4):
        pair = packed[(head // 2) * HEAD:(head // 2 + 1) * HEAD, :]
        own = jnp.where((lane < HEAD) == (head % 2 == 0), pair, 0.0)
        rows.append(jnp.concatenate([own, zero] if head < 2 else [zero, own], axis=1))
    return jnp.concatenate(rows, axis=0)


def fused_kernel(devs, scale, flag_ref, x_ref, dy_ref, wq_ref, wk_ref, wv_ref, wo_ref,
                 out_ref, y_ref, dx_ref,
                 xy, wbuf, qt, kt, vt, dt, mt, pre_in, nt, s_got, s_in, r_in, s_out, r_out, bound_ref, raw, lhs, ot, part, acc, inbox, y_acc, dx_acc, row_out,
                 xy_sem, w_sem, row_sem, pre_send, pre_recv, side_send, chain_send, chain_recv, pair_send, pair_recv, rs_send, rs_recv,
                 ag_send, ag_recv, fin_sem, peer_send, peer_recv):
    width, toks = qt.shape
    nquad = width // QUAD
    nblk = toks // BLK
    seg = QUAD
    count = 4 * nquad
    chips = devs // 2
    half = seg // 2
    side = seg // 4
    piece = side // chips
    me = lax.axis_index('sp')
    core = lax.rem(me, 2)
    chip = me // 2
    partner = chip * 2 + 1 - core
    targets = (lax.rem(chip + 1, chips) * 2 + core, lax.rem(chip + chips - 1, chips) * 2 + core)
    down = lax.rem(me + devs - 1, devs)

    load_x = pltpu.make_async_copy(x_ref, xy.at[1], xy_sem.at[1])
    load_dy = pltpu.make_async_copy(dy_ref, xy.at[0], xy_sem.at[0])
    load_x.start()

    weights = (wk_ref, wv_ref, wq_ref, wo_ref)

    def w_copy(quad, which):
        slot = lax.rem(quad, 2)
        return pltpu.make_async_copy(weights[which].at[pl.ds(pl.multiple_of(quad * QUAD, QUAD), QUAD)], wbuf.at[slot, which],
                                     w_sem.at[slot, which])

    def start_w(quad, which):
        @pl.when(quad < nquad)
        def _():
            w_copy(quad, which).start()

    start_w(jnp.int32(0), 0)
    start_w(jnp.int32(0), 1)
    start_w(jnp.int32(0), 2)
    start_w(jnp.int32(0), 3)
    load_dy.start()

    barrier = pltpu.get_barrier_semaphore()
    cross = tuple(lax.rem(chip + hop, chips) * 2 + 1 - core for hop in (1, chips - 1))
    for dev in (partner,) + targets + cross:
        pl.semaphore_signal(barrier, inc=1, device_id={'sp': dev}, device_id_type=MESH)

    lane = lax.broadcasted_iota(jnp.int32, (8, toks), 1)
    last = jnp.where(jnp.broadcast_to(flag_ref[...], (8, toks)) > 0, lane.astype(F32), -1.0)
    step = 1
    while step < toks:
        last = jnp.maximum(last, jnp.where(lane >= step, pltpu.roll(last, step, 1), -1.0))
        step *= 2
    bound_ref[...] = last
    bound = bound_ref[0:1, :]
    last_bound = jnp.max(bound, axis=1, keepdims=True)
    pos = lax.broadcasted_iota(jnp.int32, (1, toks), 1).astype(F32)
    gate = jnp.where(last_bound < 0.0, 1.0, 0.0)
    diag = (lax.broadcasted_iota(jnp.int32, (BLK, BLK), 0) <= lax.broadcasted_iota(jnp.int32, (BLK, BLK), 1))
    row_id = lax.broadcasted_iota(jnp.int32, (BLK, BLK), 0).astype(F32)

    pl.semaphore_wait(barrier, 5)
    load_x.wait()

    def quad_rows(quad):
        return pl.ds(pl.multiple_of(quad * QUAD, QUAD), QUAD)

    def pack_rows(quad):
        return pl.ds(pl.multiple_of(quad * (QUAD // 2), QUAD // 2), QUAD // 2)

    def project_kv(quad):
        slot = lax.rem(quad, 2)
        for which in range(2):
            w_copy(quad, which).wait()
            start_w(quad + 1, which)
        x_val = xy[1]
        k_val = mm(wbuf[slot, 0], x_val, NT).astype(BF16)
        kt[quad_rows(quad), :] = k_val
        v_raw = mm(wbuf[slot, 1], x_val, NT)
        vt[quad_rows(quad), :] = v_raw.astype(BF16)
        tail = pos >= last_bound
        mt[quad, 0:QUAD // 2, :] = pack_states(mm(jnp.where(tail, v_raw, 0.0).astype(BF16), k_val, NT))
        mt[quad, QUAD // 2:, :] = jnp.broadcast_to(gate, (8, 2 * HEAD))

        @pl.when(core == 0)
        def _():
            pre_copy(quad).start()

    def project_q(quad):
        w_copy(quad, 2).wait()
        start_w(quad + 1, 2)
        qt[quad_rows(quad), :] = mm(wbuf[lax.rem(quad, 2), 2], xy[1], NT).astype(BF16)

    def project_d(quad):
        w_copy(quad, 3).wait()
        start_w(quad + 1, 3)
        d_raw = mm(wbuf[lax.rem(quad, 2), 3], xy[0], NT)
        dt[quad_rows(quad), :] = d_raw.astype(BF16)
        nt[pack_rows(quad), :] = pack_states(mm(jnp.where(bound < 0.0, d_raw, 0.0).astype(BF16), qt[quad_rows(quad), :], NT))

    def pre_copy(quad):
        return pltpu.make_async_remote_copy(src_ref=mt.at[quad], dst_ref=pre_in.at[quad], send_sem=pre_send.at[quad],
                                            recv_sem=pre_recv.at[quad], device_id={'sp': partner}, device_id_type=MESH)

    def state_copy(quad, same_core):
        rows = pack_rows(quad)
        base = lax.rem(chip + 1, chips) * 2
        dev, sem = (base + 1, chain_send.at[0, quad]) if same_core else (base, side_send.at[quad])
        return pltpu.make_async_remote_copy(src_ref=s_out.at[rows], dst_ref=s_got.at[rows], send_sem=sem,
                                            recv_sem=chain_recv.at[0, quad], device_id={'sp': dev}, device_id_type=MESH)

    def state_step(quad):
        rows = pack_rows(quad)

        @pl.when(chip == 0)
        def _():
            s_got[rows, :] = jnp.zeros((QUAD // 2, 2 * HEAD), F32)

        @pl.when(chip > 0)
        def _():
            state_copy(quad, True).wait_recv()

        @pl.when(core == 0)
        def _():
            s_in[rows, :] = s_got[rows, :]

        @pl.when(core == 1)
        def _():
            pre_copy(quad).wait_recv()
            mine = pre_in[quad, QUAD // 2:QUAD // 2 + 1, :] * s_got[rows, :] + pre_in[quad, 0:QUAD // 2, :]
            s_in[rows, :] = mine

            @pl.when(chip < chips - 1)
            def _():
                s_out[rows, :] = gate * mine + mt[quad, 0:QUAD // 2, :]
                state_copy(quad, True).start()
                state_copy(quad, False).start()

    def chain_copy(quad):
        rows = pack_rows(quad)
        return pltpu.make_async_remote_copy(src_ref=r_out.at[rows], dst_ref=r_in.at[rows], send_sem=chain_send.at[1, quad],
                                            recv_sem=chain_recv.at[1, quad], device_id={'sp': down}, device_id_type=MESH)

    def chain_step(quad):
        rows = pack_rows(quad)

        @pl.when(me == devs - 1)
        def _():
            r_in[rows, :] = jnp.zeros((QUAD // 2, 2 * HEAD), F32)

        @pl.when(me < devs - 1)
        def _():
            chain_copy(quad).wait_recv()

        @pl.when(me > 0)
        def _():
            r_out[rows, :] = gate * r_in[rows, :] + nt[rows, :]
            chain_copy(quad).start()

    def remote(src, dst, s_sem, r_sem, dev):
        return pltpu.make_async_remote_copy(src_ref=src, dst_ref=dst, send_sem=s_sem, recv_sem=r_sem,
                                            device_id={'sp': dev}, device_id_type=MESH)

    def ring_idx(idx):
        return lax.rem(idx + 4 * chips, chips)

    def pair_copy(idx):
        slot = lax.rem(idx, ACC_SLOTS)
        src = part.at[lax.rem(idx, 2), pl.ds(pl.multiple_of((1 - core) * half, half), half)]
        return remote(src, acc.at[slot], pair_send.at[slot], pair_recv.at[slot], partner)

    def acc_rows(idx, way, chunk):
        return acc.at[lax.rem(idx, ACC_SLOTS), pl.ds(pl.multiple_of(way * side + chunk * piece, piece), piece)]

    def out_rows(idx, owner, way, chunk):
        row = idx * seg + owner * half + way * side + chunk * piece
        return out_ref.at[pl.ds(pl.multiple_of(row, piece), piece)]

    def sent_chunk(way, step):
        return ring_idx(chip - step if way == 0 else chip + step)

    def rs_copy(idx, way, step):
        slot = lax.rem(idx, MSG_SLOTS)
        return remote(acc_rows(idx, way, sent_chunk(way, step)), inbox.at[way, step, slot],
                      rs_send.at[way, step, slot], rs_recv.at[way, step, slot], targets[way])

    def ag_chunk(way, step):
        return ring_idx(chip + 1 - step if way == 0 else chip - 1 + step)

    def ag_copy(idx, way, step):
        slot = lax.rem(idx, MSG_SLOTS)
        rows = out_rows(idx, core, way, ag_chunk(way, step))
        src = acc_rows(idx, way, ag_chunk(way, 0)) if step == 0 else rows
        return remote(src, rows, ag_send.at[way, step, slot], ag_recv.at[way, step, slot], targets[way])

    def fin_copy(idx, way):
        chunk = ag_chunk(way, 0)
        return pltpu.make_async_copy(acc_rows(idx, way, chunk), out_rows(idx, core, way, chunk),
                                     fin_sem.at[way, lax.rem(idx, MSG_SLOTS)])

    def peer_copy(idx, way, step):
        slot = lax.rem(idx, MSG_SLOTS)
        rows = out_rows(idx, core, way, ag_chunk(way, step))
        src = acc_rows(idx, way, ag_chunk(way, 0)) if step == 0 else rows
        return remote(src, rows, peer_send.at[way, step, slot], peer_recv.at[way, step, slot], partner)


    def post_copies(idx):
        slot = lax.rem(idx, 2)
        rows = quad_rows(lax.rem(idx, nquad))
        return [pltpu.make_async_copy(ref.at[rows], wbuf.at[slot, 0], w_sem.at[slot, 0]) for ref in (wq_ref, wv_ref, wk_ref)]

    def start_post(idx):
        for kind in range(1, 4):
            @pl.when(idx // nquad == kind)
            def _():
                post_copies(idx)[kind - 1].start()

    def y_copies(idx):
        slot = lax.rem(idx, 2)
        return [pltpu.make_async_copy(wo_ref.at[quad_rows(2 * idx + i)], wbuf.at[slot, 2 + i], w_sem.at[slot, 2 + i]) for i in range(2)]

    def stage_y(idx):
        for copy in y_copies(idx):
            copy.wait()

        @pl.when(idx + 1 < nquad // 2)
        def _():
            for copy in y_copies(idx + 1):
                copy.start()
        accumulate(y_acc, [(ot.at[quad_rows(2 * idx + i)], wbuf.at[lax.rem(idx, 2), 2 + i]) for i in range(2)], idx == 0)

        @pl.when(idx == nquad // 2 - 1)
        def _():
            write_rows(y_acc, y_ref)

    def accumulate(total, terms, fresh):
        tile_t = 128

        def tile(step, carry):
            toks_at = pl.ds(pl.multiple_of(step * tile_t, tile_t), tile_t)
            add = mm(terms[0][0][:, toks_at], terms[0][1][...], TN) + mm(terms[1][0][:, toks_at], terms[1][1][...], TN)

            @pl.when(fresh)
            def _():
                total[toks_at, :] = add

            @pl.when(jnp.logical_not(fresh))
            def _():
                total[toks_at, :] += add
            return carry
        lax.fori_loop(0, toks // tile_t, tile, 0)

    def write_rows(total, dst):
        tile_t = row_out.shape[1]
        for i in range(toks // tile_t):
            copy = pltpu.make_async_copy(row_out.at[i % 2], dst.at[i * tile_t:(i + 1) * tile_t], row_sem.at[i % 2])
            if i >= 2:
                copy.wait()
            row_out[i % 2] = total[i * tile_t:(i + 1) * tile_t, :].astype(BF16)
            copy.start()
        for i in range(2):
            pltpu.make_async_copy(row_out.at[i], dst.at[i * tile_t:(i + 1) * tile_t], row_sem.at[i]).wait()

    def stage_post(idx):
        post_copies(idx)[0].wait()

        @pl.when(lax.rem(idx, 2) == 1)
        def _():
            accumulate(dx_acc, [(lhs.at[slot], wbuf.at[slot, 0]) for slot in range(2)], idx == nquad + 1)

        @pl.when(idx + 1 < count)
        def _():
            start_post(idx + 1)

        @pl.when(idx == 2 * nquad - 1)
        def _():
            for copy in y_copies(jnp.int32(0)):
                copy.start()
        turn_y = idx - 2 * nquad

        @pl.when(jnp.logical_and(lax.rem(idx, 2) == 0, jnp.logical_and(turn_y >= 0, turn_y < nquad)))
        def _():
            stage_y(turn_y // 2)

        @pl.when(idx == count - 1)
        def _():
            write_rows(dx_acc, dx_ref)

    def unit(idx, kind):
        quad = lax.rem(idx, nquad)
        slot = lax.rem(idx, 2)
        by_query = kind < 2
        left, right = (kt, qt) if kind % 2 == 0 else (vt, dt)
        value = (vt, kt, dt, qt)[kind]

        def head_step(head, carry):
            rows = pl.ds(pl.multiple_of(quad * QUAD + head * HEAD, HEAD), HEAD)
            for ob in range(nblk):
                total = None
                for ib in (range(ob + 1) if by_query else range(ob, nblk)):
                    tb, sb = (ob, ib) if by_query else (ib, ob)
                    t_cols, s_cols = pl.ds(tb * BLK, BLK), pl.ds(sb * BLK, BLK)
                    seen = row_id + float(sb * BLK) >= bound_ref[0:1, t_cols]
                    if sb == tb:
                        seen = jnp.logical_and(seen, diag)
                    prob = jnp.where(seen, mm(left[rows, s_cols], right[rows, t_cols], TN) * scale, 0.0).astype(BF16)
                    if by_query:
                        part_sum = mm(value[rows, s_cols], prob, NN)
                    else:
                        part_sum = mm(value[rows, t_cols], prob, NT)
                    total = part_sum if total is None else total + part_sum
                raw[pl.ds(pl.multiple_of(head * HEAD, HEAD), HEAD), ob * BLK:(ob + 1) * BLK] = total
            return carry

        lax.fori_loop(0, QUAD // HEAD, head_step, 0)
        state = s_in if by_query else r_in
        full = spread_states(state[pack_rows(quad), :]).astype(BF16)
        other = (qt, dt, kt, vt)[kind]
        dims = NN if kind % 2 == 0 else TN
        weight = jnp.where(bound < 0.0, scale, 0.0) if by_query else jnp.where(pos >= last_bound, scale, 0.0)
        for tb in range(nblk):
            cols = pl.ds(tb * BLK, BLK)
            extra = mm(full, other[quad_rows(quad), cols], dims) * weight[:, tb * BLK:(tb + 1) * BLK]
            lhs[slot, :, cols] = (raw[:, cols] + extra).astype(BF16)
            if kind == 0:
                ot[quad_rows(quad), cols] = lhs[slot, :, cols]

    def stage_unit(idx):
        for kind in range(4):
            @pl.when(idx // nquad == kind)
            def _():
                unit(idx, kind)

    def stage_partial(idx):
        slot = lax.rem(idx, 2)

        @pl.when(idx == 0)
        def _():
            load_dy.wait()
        rhs_id = jnp.minimum(idx // nquad, 1)
        tile_n = width // 2

        def tile(step, carry):
            cols = pl.ds(pl.multiple_of(step * tile_n, tile_n), tile_n)
            part[slot, :, cols] = mm(lhs[slot], xy[rhs_id, :, cols], NN)
            return carry
        lax.fori_loop(0, width // tile_n, tile, 0)
        pair_copy(idx).start()

        @pl.when(idx == nquad - 1)
        def _():
            start_post(idx + 1)

        @pl.when(idx >= nquad)
        def _():
            stage_post(idx)

    def add_rows(idx, way, step):
        chunk = sent_chunk(way, step)
        rows = pl.ds(pl.multiple_of(way * side + chunk * piece, piece), piece)
        slot = lax.rem(idx, ACC_SLOTS)
        acc[slot, rows, :] = acc[slot, rows, :] + inbox[way, step - 1, lax.rem(idx, MSG_SLOTS)]

    def stage_pair(idx):
        copy = pair_copy(idx)
        copy.wait()
        slot = lax.rem(idx, ACC_SLOTS)

        def add(step, carry):
            rows = pl.ds(pl.multiple_of(step * piece, piece), piece)
            own = pl.ds(pl.multiple_of(core * half + step * piece, piece), piece)
            acc[slot, rows, :] = acc[slot, rows, :] + part[lax.rem(idx, 2), own, :]
            return carry
        lax.fori_loop(0, half // piece, add, 0)
        for way in range(2):
            rs_copy(idx, way, 0).start()

    def stage_reduce(idx, step):
        for way in range(2):
            prev = rs_copy(idx, way, step - 1)
            prev.wait_send()
            prev.wait_recv()
            add_rows(idx, way, step)
            if step < chips - 1:
                rs_copy(idx, way, step).start()
            else:
                ag_copy(idx, way, 0).start()
                peer_copy(idx, way, 0).start()
                fin_copy(idx, way).start()

    def stage_gather(idx, step):
        for way in range(2):
            ag_copy(idx, way, step).wait_send()
            slot = lax.rem(idx, MSG_SLOTS)
            got = out_rows(idx, core, way, ag_chunk(way, step + 1))
            remote(got, got, ag_send.at[way, step, slot], ag_recv.at[way, step, slot], targets[way]).wait_recv()
            if step + 1 < chips - 1:
                ag_copy(idx, way, step + 1).start()
            peer_copy(idx, way, step + 1).start()
            if step == 0:
                fin_copy(idx, way).wait()
            finish_peer(idx, way, step)

    def finish_peer(idx, way, step):
        peer_copy(idx, way, step).wait_send()
        slot = lax.rem(idx, MSG_SLOTS)
        got = out_rows(idx, 1 - core, way, ag_chunk(way, step))
        remote(got, got, peer_send.at[way, step, slot], peer_recv.at[way, step, slot], partner).wait_recv()

    def stage_last(idx):
        for way in range(2):
            finish_peer(idx, way, chips - 1)

    order = [(2 * chips, stage_last)]
    for step in reversed(range(chips - 1)):
        order.append((chips + 1 + step, functools.partial(stage_gather, step=step)))
    for step in reversed(range(1, chips)):
        order.append((1 + step, functools.partial(stage_reduce, step=step)))
    order.append((1, stage_pair))
    lead = chips

    def when_in(idx, limit, body):
        @pl.when(jnp.logical_and(idx >= 0, idx < limit))
        def _():
            body(idx)

    def tick_step(tick, carry):
        when_in(tick, nquad, project_kv)
        when_in(tick - lead, nquad, project_q)
        when_in(tick - lead - LATE, nquad, project_d)
        when_in(tick - 1 - chip, nquad, state_step)
        when_in(tick - lead - LATE - (devs - 1 - me), nquad, chain_step)
        rnd = tick - lead

        def poll(turn, carry):
            for delay, stage in order:
                slow = rnd - delay
                quick = rnd - (delay + 1) // 2
                on_turn = turn == (0 if delay % 2 else 1)
                is_quick = jnp.logical_and(on_turn, jnp.logical_and(quick >= 0, quick < FAST))
                is_slow = jnp.logical_and(turn == 0, jnp.logical_and(slow >= FAST, slow < count))

                @pl.when(jnp.logical_or(is_quick, is_slow))
                def _():
                    stage(jnp.where(is_quick, quick, slow))

            @pl.when(turn == 0)
            def _():
                when_in(rnd, count, stage_unit)

            @pl.when(turn == 1)
            def _():
                when_in(rnd, count, stage_partial)
            return carry
        lax.fori_loop(0, 2, poll, 0)
        return carry

    lax.fori_loop(0, lead + count + 2 * chips, tick_step, 0)

    def chain_end(quad, carry):
        @pl.when(core == 0)
        def _():
            pre_copy(quad).wait_send()

        @pl.when(jnp.logical_and(core == 1, chip < chips - 1))
        def _():
            state_copy(quad, True).wait_send()
            state_copy(quad, False).wait_send()

        @pl.when(me > 0)
        def _():
            chain_copy(quad).wait_send()
        return carry
    lax.fori_loop(0, nquad, chain_end, 0)


def fused(devs, scale, flags, x_loc, dy_loc, wq, wk, wv, wo):
    toks, width = x_loc.shape
    chips = devs // 2
    nquad = width // QUAD
    piece = QUAD // 4 // chips
    dma = pltpu.SemaphoreType.DMA
    act = jax.ShapeDtypeStruct((toks, width), BF16)
    state = pltpu.VMEM((width // 2, 2 * HEAD), F32)
    ring = (2, chips - 1, MSG_SLOTS)
    return pl.pallas_call(
        functools.partial(fused_kernel, devs, scale),
        name='fused',
        in_specs=[pl.BlockSpec(memory_space=pltpu.VMEM)] + [pl.BlockSpec(memory_space=pl.ANY)] * 6,
        out_specs=[pl.BlockSpec(memory_space=pl.ANY)] * 3,
        out_shape=[jax.ShapeDtypeStruct((4 * width, width), F32)] + [act] * 2,
        scratch_shapes=[
            pltpu.VMEM((2, toks, width), BF16),
            pltpu.VMEM((2, 4, QUAD, width), BF16),
            *[pltpu.VMEM((width, toks), BF16)] * 4,
            pltpu.VMEM((nquad, QUAD // 2 + 8, 2 * HEAD), F32),
            pltpu.VMEM((nquad, QUAD // 2 + 8, 2 * HEAD), F32),
            *[state] * 6,
            pltpu.VMEM((8, toks), F32),
            pltpu.VMEM((QUAD, toks), F32),
            pltpu.VMEM((2, QUAD, toks), BF16),
            pltpu.VMEM((width, toks), BF16),
            pltpu.VMEM((2, QUAD, width), F32),
            pltpu.VMEM((ACC_SLOTS, QUAD // 2, width), F32),
            pltpu.VMEM((2, chips - 1, MSG_SLOTS, piece, width), F32),
            pltpu.VMEM((toks, width), F32),
            pltpu.VMEM((toks, width), F32),
            pltpu.VMEM((2, 128, width), BF16),
            dma((2,)), dma((2, 4)), dma((2,)), dma((nquad,)), dma((nquad,)), dma((nquad,)), dma((2, nquad)), dma((2, nquad)), dma((ACC_SLOTS,)), dma((ACC_SLOTS,)),
            dma(ring), dma(ring), dma(ring), dma(ring), dma((2, MSG_SLOTS)),
            dma((2, chips, MSG_SLOTS)), dma((2, chips, MSG_SLOTS)),
        ],
        compiler_params=pltpu.CompilerParams(vmem_limit_bytes=VMEM_CAP, collective_id=0, has_side_effects=True),
        cost_estimate=pl.CostEstimate(flops=24 * toks * width * width, bytes_accessed=150 * 1024 * 1024, transcendentals=0),
    )(flags.reshape(1, toks), x_loc, dy_loc, wq, wk, wv, wo)


def solution(mesh):
    devs = mesh.shape['sp']

    def device_body(x_loc, flag_loc, w_q, w_k, w_v, w_o, dy_loc):
        toks, width = x_loc.shape
        heads, head_dim = w_q.shape[1], w_q.shape[2]
        scale = 1.0 / (math.sqrt(head_dim) * toks)
        wq, wk, wv = [jnp.transpose(w, (1, 2, 0)).reshape(width, width) for w in (w_q, w_k, w_v)]
        wo = w_o.reshape(width, width)
        total, y_loc, dx_loc = fused(devs, scale, flag_loc, x_loc, dy_loc, wq, wk, wv, wo)
        dw_o, dw_q, dw_v, dw_k = [total[i * width:(i + 1) * width].reshape(heads, head_dim, width) for i in range(4)]
        dw_q, dw_k, dw_v = [jnp.transpose(dw, (2, 0, 1)) for dw in (dw_q, dw_k, dw_v)]
        return y_loc, dx_loc, dw_q, dw_k, dw_v, dw_o

    row_spec = P(('dp', 'sp'), None)
    flag_spec = P(('dp', 'sp'))
    w_spec = P(None, None, None)
    dw_spec = P('dp', None, None)
    return jax.shard_map(device_body, mesh=mesh,
                         in_specs=(row_spec, flag_spec, w_spec, w_spec, w_spec, w_spec, row_spec),
                         out_specs=(row_spec, row_spec, dw_spec, dw_spec, dw_spec, dw_spec),
                         check_vma=False)
```
